32 devices in a mesh: gx: 2 (over x), gy: 4 (over y, core), gz: 4 (over z).
Axes of the slice: x: 2, y: 2, z: 4, core: 2. Of those that a mesh axis runs over, the one named last changes fastest.
Arguments:
- fields: float32 [6, 32, 64, 512], P(None, 'gx', 'gy', 'gz'), may hold values from -6 to 6
- permittivity: float32 [32, 64, 512], P('gx', 'gy', 'gz'), may hold values from 1 to 4
- donor_owner: int32 [4096, 1], P(('gx', 'gy', 'gz')), may hold values from 0 to 15; in each aligned block of 128 rows (0 to 127, 128 to 255, ...) at most 16 rows name the same one
- donor_base: int32 [4096, 3], P(('gx', 'gy', 'gz')), may hold values from 0 to 127, as said below
- donor_weights: float32 [4096, 15], P(('gx', 'gy', 'gz')), may hold values from -3 to 3
Outputs:
- new_fields: float32 [6, 32, 64, 512], P(None, 'gx', 'gy', 'gz')
- receptor_values: float32 [6, 4096], P(None, ('gx', 'gy', 'gz'))
The draws below stay inside these ranges and needn't reach their ends.
Inputs may be any that keep to these rules, and one draw needn't show every extreme that they name: `donor_owner`: within the 128 rows of one device no owner index is named by more than 16 rows, and one is named by exactly 16. `donor_base`: column 0 lies in 0 to 15, column 1 in 0 to 15, column 2 in 0 to 127.
All inputs are finite; a program needn't handle non-finite values.
Results may differ from the reference program's by a relative error of at most 0.00002.
Values sent between devices are 32-bit elements; how exact they have to be, the bound alone decides.
A program may use at most 192 MiB of HBM per device.

```python
import math
import jax
import jax.numpy as jnp
import numpy as np
from jax import lax

CX = 16
CY = 16
CZ = 128
R_DEV = 128
CAP = 16
NX = 32
NY = 64
NZ = 512
RECEPT = 4096
N_GY = 4
N_GZ = 4
DEVICES = 32


def draw_donor_base(key, part):
    first = jax.random.randint(jax.random.fold_in(key, 11), (RECEPT, 1), 0, CX, dtype=jnp.int32)
    second = jax.random.randint(jax.random.fold_in(key, 12), (RECEPT, 1), 0, CY, dtype=jnp.int32)
    third = jax.random.randint(jax.random.fold_in(key, 13), (RECEPT, 1), 0, CZ, dtype=jnp.int32)
    return jnp.concatenate([first, second, third], 1)


def steps_of(rng, extent, pieces, low, largest):
    gain, own = 1.0, jax.random.fold_in(rng, 6)
    for position, blocks in pieces:
        heights = jnp.exp(jax.random.uniform(jax.random.fold_in(own, position), (blocks,), jnp.float32, low / len(pieces), largest / len(pieces)))
        gain = gain * jnp.repeat(heights, extent[position] // blocks).reshape([-1 if axis == position else 1 for axis in range(len(extent))])
    return gain


def shared_out(stream_key, own, number, rows, amount, top, most, lean):
    sequence = jax.random.permutation(stream_key, amount)
    packed, common = shares(amount, rows * top, most, lean, True), shares(amount, rows * top, most, lean, False)
    places = jnp.arange(amount)

    def named(tallies, offset_by):
        used = int((tallies > 0).sum())
        fixed = max(1, used // 4)
        passed = fixed + (places - fixed + offset_by * (used - fixed)) % max(1, amount - fixed)
        return jnp.zeros((amount,), jnp.int32).at[sequence[jnp.where(places < fixed, places, passed)]].set(jnp.asarray(tallies, jnp.int32))

    tallies = jnp.where(number % 4 == 0, named(packed, number // 4), named(common, number - number // 4 - 1))
    mixed = jax.random.permutation(jax.random.fold_in(own, 3), amount)
    source_of, sink = mixed[0:amount // 2 * 2:2], mixed[1:amount // 2 * 2:2]
    room = jnp.minimum(tallies[source_of] - 1, most - tallies[sink]) // 2
    room = jnp.where((source_of == sequence[0]) | (sink == sequence[0]) | (tallies[sink] == 0), 0, jnp.maximum(room, 0))
    passed = jax.random.randint(jax.random.fold_in(own, 4), (amount // 2,), 0, 1 << 20) % (room + 1)
    tallies = tallies.at[source_of].add(-passed).at[sink].add(passed)
    labels = jnp.searchsorted(jnp.cumsum(tallies), jnp.arange(rows * top), side="right").astype(jnp.int32)
    grid = labels.reshape(top, rows).T
    grid = grid[jax.random.permutation(jax.random.fold_in(own, 1), rows)]
    offset_by = jax.random.randint(jax.random.fold_in(own, 2), (rows, 1), 0, top)
    return jnp.take_along_axis(grid, (jnp.arange(top)[None, :] + offset_by) % top, axis=1)


def shares(number_of, total, limit, slope, full):
    portions = [(1 << 20) // math.isqrt(standing ** slope) + 1 for standing in range(1, number_of + 1)]
    largest = limit if full else min(limit, max(-(-total // number_of), total * portions[0] // sum(portions)))
    least = 1 if total - largest >= number_of - 1 else 0
    holding, spare = [largest] + [least] * (number_of - 1), total - largest - least * (number_of - 1)
    while spare > 0:
        movable = [i for i in range(1, number_of) if holding[i] < largest] or [i for i in range(1, number_of) if holding[i] < limit]
        whole, budget = sum([portions[i] for i in movable]), spare
        for i in movable:
            addition = min(limit - holding[i], max(1, budget * portions[i] // whole), spare)
            holding[i] = holding[i] + addition
            spare = spare - addition
    return np.array(holding)


def bell_draw(own_key, shape, scale, most, cuts=(), kind=jnp.bfloat16):
    loudness = steps_of(own_key, shape, cuts, -0.22, 0.18) if cuts else 1.0
    values = jax.random.normal(own_key, shape, jnp.float32) * scale * loudness
    return jnp.minimum(jnp.maximum(values, -most), most).astype(kind)


def setup_inputs(seed: int = 0) -> dict:
    streams_of = jax.random.split(jax.random.key(seed), 6)
    fields = bell_draw(streams_of[0], (6, NX, NY, NZ), 1.0, 6.0, ((1, 2), (2, 4), (3, 4)), jnp.float32)
    permittivity = jnp.clip(jnp.exp(math.log(4.0) - 1.3862944 * jax.random.uniform(streams_of[1], (NX, NY, NZ), jnp.float32) ** steps_of(streams_of[1], (NX, NY, NZ), ((0, 2), (1, 4), (2, 4)), -0.2, 0.2)), 1.0, 4.0)
    donor_owner_keys = jax.random.split(jax.random.fold_in(streams_of[2], 1), RECEPT // R_DEV)
    donor_owner_turns = jax.random.permutation(jax.random.fold_in(streams_of[2], 3), RECEPT // R_DEV)
    donor_owner = jax.vmap(lambda own, number: shared_out(jax.random.fold_in(streams_of[2], 2), own, number, R_DEV, N_GY * N_GZ, 1, CAP, 2))(donor_owner_keys, donor_owner_turns).reshape((RECEPT, 1))
    donor_base = draw_donor_base(jax.random.fold_in(streams_of[5], 71), 0)
    donor_weights = bell_draw(streams_of[4], (RECEPT, 15), 0.5, 3.0, ((0, 32),), jnp.float32)
    return {"fields": fields, "permittivity": permittivity, "donor_owner": donor_owner, "donor_base": donor_base, "donor_weights": donor_weights}


step_size = 0.25


def shifted(field, axis_index, offset):
    window = [slice(2, -2), slice(2, -2), slice(2, -2)]
    length = field.shape[axis_index] - 4
    window[axis_index] = slice(2 + offset, 2 + offset + length)
    return field[tuple(window)]


def derivative(field, axis_index):
    outer = shifted(field, axis_index, -2) - shifted(field, axis_index, 2)
    inner = shifted(field, axis_index, 1) - shifted(field, axis_index, -1)
    return (outer + 8.0 * inner) / 12.0


def curl_rate(padded, coefficient):
    rate_ex = (derivative(padded[5], 1) - derivative(padded[4], 2)) / coefficient
    rate_ey = (derivative(padded[3], 2) - derivative(padded[5], 0)) / coefficient
    rate_ez = (derivative(padded[4], 0) - derivative(padded[3], 1)) / coefficient
    rate_hx = derivative(padded[1], 2) - derivative(padded[2], 1)
    rate_hy = derivative(padded[2], 0) - derivative(padded[0], 2)
    rate_hz = derivative(padded[0], 1) - derivative(padded[1], 0)
    return jnp.stack([rate_ex, rate_ey, rate_ez, rate_hx, rate_hy, rate_hz])


def contract(donor_tiles, weights):
    weight_x = weights[0:5]
    weight_y = weights[5:10]
    weight_z = weights[10:15]
    along_z = jnp.sum(donor_tiles * weight_z[None, None, None, :, :], axis=3)
    along_y = jnp.sum(along_z * weight_y[None, None, :, :], axis=2)
    return jnp.sum(along_y * weight_x[None, :, :], axis=1)


def reference(fields, permittivity, donor_owner, donor_base, donor_weights):
    accumulated = fields
    taylor_term = fields
    for power in range(1, 5):
        padded = jnp.pad(taylor_term, ((0, 0), (2, 2), (2, 2), (2, 2)))
        taylor_term = (step_size / power) * curl_rate(padded, permittivity)
        accumulated = accumulated + taylor_term
    new_fields = accumulated
    donor_grid = jnp.pad(new_fields, ((0, 0), (2, 2), (2, 2), (2, 2)))
    group_size = N_GY * N_GZ
    device_id = jnp.arange(RECEPT, dtype=jnp.int32) // R_DEV
    plane_id = device_id // group_size
    owner_id = donor_owner[:, 0].astype(jnp.int32)
    row_x = plane_id * CX + donor_base[:, 0]
    row_y = (owner_id // N_GZ) * CY + donor_base[:, 1]
    row_z = (owner_id % N_GZ) * CZ + donor_base[:, 2]
    corners = jnp.stack([row_x, row_y, row_z], 1).astype(jnp.int32).reshape(DEVICES, R_DEV, 3)
    weights = donor_weights.reshape(DEVICES, R_DEV, 15)

    def one_block(block_item):
        corner_rows, weight_rows = block_item
        donor_tiles = jax.vmap(
            lambda corner: lax.dynamic_slice(donor_grid, (jnp.int32(0), corner[0], corner[1], corner[2]), (6, 5, 5, 5)),
            out_axes=4)(corner_rows)
        return contract(donor_tiles, weight_rows.T)

    values = lax.map(one_block, (corners, weights))
    receptor_values = jnp.transpose(values, (1, 0, 2)).reshape(6, RECEPT)
    return new_fields, receptor_values
```

```python
import functools

import jax
import jax.numpy as jnp
from jax import lax
from jax.experimental import pallas as pl
from jax.experimental.pallas import tpu as pltpu
from jax.sharding import PartitionSpec as P

step_size = 0.25
MESH = pl.DeviceIdType.MESH
F32 = jnp.float32
BF16 = jnp.bfloat16
HI = lax.Precision.HIGHEST
BLOCKS = 4
FEATURES = 32
DIRS = [(a, b, c) for a in (-1, 0, 1) for b in (-1, 0, 1) for c in (-1, 0, 1) if (a, b, c) != (0, 0, 0)]
FACES = [(-1, 0, 0), (1, 0, 0), (0, -1, 0), (0, 1, 0), (0, 0, -1), (0, 0, 1)]


def dot(a, b, dims=((1,), (0,))):
    return lax.dot_general(a, b, (dims, ((), ())), precision=HI, preferred_element_type=F32)


def split(a):
    hi = a.astype(BF16)
    return hi, (a - hi.astype(F32)).astype(BF16)


def dot16(a, b):
    return lax.dot_general(a, b, (((1,), (0,)), ((), ())), preferred_element_type=F32)


def negate(way):
    return tuple(-a for a in way)


def slot_of(a):
    return 0 if a < 0 else 1


def kernel(
    sizes, fields, eps, owner_in, bases_in, weights_in, out, recept,
    owner, bases, weights, T, F, inv, ys, yr, zs, zr, DZ,
    yfs, zfs, XR, YR, XYR, ZR, ZX, ZY, ZXY,
    data_t, inner, req, reqr, ans, ansr, W, W_lo, V, V_lo, Wy, wzx, wz_in, hits_s, slot_s, part,
    load_sem, send, recv, fsend, frecv, rsend, rrecv, asend, arecv,
):
    nx, ny, nz, cap = sizes
    group = ny * nz
    per_owner = cap // BLOCKS
    cx, cy, cz = eps.shape
    rows = owner.shape[1]
    slots = group * cap
    x, y, z = lax.axis_index("gx"), lax.axis_index("gy"), lax.axis_index("gz")
    me = y * nz + z
    y0, y1 = 8, 8 + cy

    loads = [
        pltpu.make_async_copy(fields, T.at[0, :, pl.ds(2, cx), pl.ds(8, cy), :], load_sem.at[0]),
        pltpu.make_async_copy(owner_in, owner, load_sem.at[1]),
        pltpu.make_async_copy(bases_in, bases, load_sem.at[2]),
        pltpu.make_async_copy(weights_in, weights, load_sem.at[3]),
        pltpu.make_async_copy(eps, inv, load_sem.at[4]),
        pltpu.make_async_copy(fields, F, load_sem.at[5]),
    ]
    for copy in loads:
        copy.start()

    has = {
        (-1, 0, 0): x > 0, (1, 0, 0): x < nx - 1, (0, -1, 0): y > 0,
        (0, 1, 0): y < ny - 1, (0, 0, -1): z > 0, (0, 0, 1): z < nz - 1,
    }
    for way in DIRS:
        found = None
        for axis in range(3):
            if way[axis]:
                face = tuple(way[a] if a == axis else 0 for a in range(3))
                found = has[face] if found is None else found & has[face]
        has[way] = found

    def dev(way):
        return (x + way[0], y + way[1], z + way[2])

    barrier = pltpu.get_barrier_semaphore()
    others = []
    for d in range(1, group):
        t = lax.rem(me + d, group)
        others.append((x, t // nz, lax.rem(t, nz)))
    expected = jnp.int32(group - 1)
    for way in DIRS:
        if way[0]:
            expected = expected + has[way].astype(jnp.int32)

            @pl.when(has[way])
            def _():
                pl.semaphore_signal(barrier, inc=1, device_id=dev(way), device_id_type=MESH)
    for target in others:
        pl.semaphore_signal(barrier, inc=1, device_id=target, device_id_type=MESH)

    def clear(ref):
        ref[...] = jnp.zeros(ref.shape, F32)

    for way in DIRS:
        kx, ky, kz = (slot_of(a) for a in way)
        here = tuple(abs(a) for a in way)

        @pl.when(jnp.logical_not(has[way]))
        def _():
            if here == (1, 0, 0):
                for m in range(4):
                    clear(T.at[m, :, pl.ds(kx * (cx + 2), 2), pl.ds(8, cy)])
                clear(XR.at[:, kx])
            elif here == (0, 1, 0):
                clear(yr.at[:, ky])
                clear(YR.at[:, ky])
            elif here == (0, 0, 1):
                clear(zr.at[:, kz])
                clear(ZR.at[:, kz])
            elif here == (1, 1, 0):
                clear(XYR.at[:, kx, ky])
            elif here == (1, 0, 1):
                clear(ZX.at[:, kx, kz])
            elif here == (0, 1, 1):
                clear(ZY.at[:, ky, kz])
            else:
                clear(ZXY.at[:, kx, ky, kz])

    zi = lax.broadcasted_iota(jnp.int32, (2 * cz, cz), 0) % cz
    zo = lax.broadcasted_iota(jnp.int32, (2 * cz, cz), 1)
    delta = zi - zo
    inner[...] = (jnp.where(delta == -2, 1.0, 0.0) - jnp.where(delta == 2, 1.0, 0.0)
                  + jnp.where(delta == 1, 8.0, 0.0) - jnp.where(delta == -1, 8.0, 0.0)).astype(BF16)

    lane = lax.broadcasted_iota(jnp.int32, (cy, cz), 1)
    lane1 = lax.broadcasted_iota(jnp.int32, (1, cz), 1)

    def remote(src, dst, s, r, target):
        return pltpu.make_async_remote_copy(
            src_ref=src, dst_ref=dst, send_sem=s, recv_sem=r, device_id=target, device_id_type=MESH)

    def request(d):
        return remote(req.at[(me + d) % group], reqr.at[me], rsend.at[d], rrecv.at[d], others[d - 1])

    def answer(d):
        return remote(ans.at[(me + d) % group], ansr.at[me], asend.at[d], arecv.at[d], others[d - 1])

    def parts(h):
        m = h // 2
        sp = (m + h % 2) % 2
        return m, sp, 3 * (1 - sp), 3 * sp

    def face_copy(h, way):
        m, sp, s, d = parts(h)
        i = FACES.index(way)
        if way[0]:
            lo_src, lo_dst = (2, cx + 2) if way[0] < 0 else (cx, 0)
            src = T.at[m, pl.ds(s + 1, 2), pl.ds(lo_src, 2), pl.ds(8, cy)]
            dst = T.at[m, pl.ds(s + 1, 2), pl.ds(lo_dst, 2), pl.ds(8, cy)]
        elif way[1]:
            k = slot_of(way[1])
            src, dst = ys.at[h, k], yr.at[h, 1 - k]
        else:
            src, dst = zs.at[h], zr.at[h, 1 - slot_of(way[2])]
        return remote(src, dst, send.at[h, i], recv.at[h, i], dev(way))

    def start_face(h, ways):
        for way in ways:
            @pl.when(has[way])
            def _():
                face_copy(h, way).start()

    def recv_face(h, ways):
        for way in ways:
            @pl.when(has[negate(way)])
            def _():
                face_copy(h, way).wait_recv()

    XW, YW, ZW = FACES[0:2], FACES[2:4], FACES[4:6]
    per = cz // 8

    def pack_y(h):
        m, sp, s, d = parts(h)
        for q, c in enumerate((0, 2)):
            ys[h, 0, :, 2 * q:2 * q + 2, :] = T[m, s + c, 2:2 + cx, y0:y0 + 2, :]
            ys[h, 1, :, 2 * q:2 * q + 2, :] = T[m, s + c, 2:2 + cx, y1 - 2:y1, :]

    def pack_z(h):
        m, sp, s, d = parts(h)
        for g in range(cx // per):
            strip = jnp.zeros((cy, cz), F32)
            for i in range(per):
                for q in range(2):
                    b = i * 8 + q * 4
                    strip = jnp.where(lane // 4 == b // 4,
                                      pltpu.roll(T[m, s + q, 2 + g * per + i, y0:y1, :], (b + 2) % cz, 1), strip)
            zs[h, g] = strip

    loads[0].wait()
    for h in range(2):
        pack_y(h)
        pack_z(h)
    pl.semaphore_wait(barrier, expected)
    for h in range(2):
        start_face(h, XW + YW + ZW)

    for copy in loads[1:4]:
        copy.wait()
    data_t[...] = jnp.zeros(data_t.shape, F32)
    for b in range(BLOCKS):
        at = b * FEATURES
        data_t[at:at + 3] = bases[...].astype(F32)
        data_t[at + 3:at + 18] = weights[...]
        data_t[at + 18:at + 19] = owner[...].astype(F32)
    data = jnp.transpose(data_t[...])
    col = lax.broadcasted_iota(jnp.int32, (rows, 128), 1)
    own = data[:, 18:19].astype(jnp.int32)
    hits = (own == col).astype(F32)
    hits_s[...] = hits
    earlier = dot16((lax.broadcasted_iota(jnp.int32, (rows, rows), 1)
                     < lax.broadcasted_iota(jnp.int32, (rows, rows), 0)).astype(BF16), hits.astype(BF16))
    slot = jnp.sum(earlier * hits, axis=1, keepdims=True).astype(jnp.int32)
    slot_s[...] = jnp.broadcast_to(slot, slot_s.shape)
    placed = jnp.where(col // FEATURES == slot // per_owner, data, 0.0)
    flat = own * per_owner + slot % per_owner
    perm = (flat == lax.broadcasted_iota(jnp.int32, (rows, group * per_owner), 1)).astype(F32)
    packed = dot(perm, placed, ((0,), (0,)))
    for o in range(group):
        req[o] = packed[o * per_owner:(o + 1) * per_owner]
    reqr[me] = req[me]
    for d in range(1, group):
        request(d).start()

    loads[4].wait()
    inv[...] = 1.0 / (12.0 * inv[...])
    loads[5].wait()

    edge = (lane < 2) | (lane >= cz - 2)
    tail = lane % 4

    def final_copy(j, way):
        i = DIRS.index(way)
        d = 3 * (1 - j)
        here = tuple(abs(a) for a in way)
        kx, ky, kz = (slot_of(a) for a in way)
        nx_, ny_, nz_ = 1 - kx, 1 - ky, 1 - kz
        strip = kx * (zfs.shape[1] - 1)
        if here == (1, 0, 0):
            src, dst = F.at[pl.ds(d, 3), pl.ds(kx * (cx - 2), 2)], XR.at[pl.ds(d, 3), nx_]
        elif here == (0, 1, 0):
            src, dst = yfs.at[j, ky], YR.at[pl.ds(d, 3), ny_]
        elif here == (0, 0, 1):
            src, dst = zfs.at[j], ZR.at[j, nz_]
        elif here == (1, 1, 0):
            src = yfs.at[j, ky, :, pl.ds(kx * (2 * cx - 8), 8)]
            dst = XYR.at[pl.ds(d, 3), nx_, ny_]
        elif here == (1, 0, 1):
            src, dst = zfs.at[j, strip], ZX.at[j, nx_, nz_]
        elif here == (0, 1, 1):
            src, dst = zfs.at[j, :, pl.ds(ky * (cy - 8), 8)], ZY.at[j, ny_, nz_]
        else:
            src, dst = zfs.at[j, strip, pl.ds(ky * (cy - 8), 8)], ZXY.at[j, nx_, ny_, nz_]
        return remote(src, dst, fsend.at[j, i], frecv.at[j, i], dev(way))

    def start_final(j, ways):
        for way in ways:
            @pl.when(has[way])
            def _():
                final_copy(j, way).start()

    wide = cz // 16

    def send_final(j):
        d = 3 * (1 - j)
        start_final(j, XW)
        for k, lo in ((0, 0), (1, cy - 2)):
            for c in range(3):
                for px in range(cx):
                    yfs[j, k, c, 2 * px:2 * px + 2, :] = F[d + c, px, lo:lo + 2, :]
        start_final(j, YW + [way for way in DIRS if way[0] and way[1] and not way[2]])
        for g in range(cx // wide):
            strip = jnp.zeros((cy, cz), F32)
            for i in range(wide):
                for c in range(3):
                    b = i * 16 + c * 4
                    strip = jnp.where(lane // 4 == b // 4,
                                      pltpu.roll(F[d + c, g * wide + i], (b + 2) % cz, 1), strip)
            zfs[j, g] = strip
        start_final(j, [way for way in DIRS if way[2]])

    served_rows = group * per_owner

    def served_table():
        if per_owner % 8 == 0:
            table = reqr[...].reshape(served_rows, 128)
        else:
            table = jnp.concatenate([reqr[o] for o in range(group)], axis=0)
        turned = [table] + [pltpu.roll(table, 128 - b * FEATURES, 1) for b in range(1, BLOCKS)]
        return jnp.concatenate(turned, axis=0)

    def spread(served, at, base, first):
        offset = at - base
        total = jnp.zeros(offset.shape, F32)
        for k in range(5):
            total = jnp.where(offset == k, served[:, first + k:first + k + 1], total)
        return total

    def corner(served, axis):
        return served[:, axis:axis + 1].astype(jnp.int32)

    def build_inner():
        for d in range(1, group):
            request(d).wait_recv()
        served = served_table()
        bx, by = corner(served, 0), corner(served, 1)
        for lo in range(0, cx * cy, 128):
            li = lo + lax.broadcasted_iota(jnp.int32, (1, 128), 1)
            both = spread(served, li // cy + 2, bx, 3) * spread(served, li % cy + 2, by, 8)
            W[:, lo:lo + 128], W_lo[:, lo:lo + 128] = split(both)

    def build_outer():
        served = served_table()
        bx, by = corner(served, 0), corner(served, 1)
        nxr, nyr = 4 * cy, 4 * cx
        for lo in range(0, V.shape[1], 128):
            li = lo + lax.broadcasted_iota(jnp.int32, (1, 128), 1)
            i1 = li % (2 * cy)
            xa = i1 // cy + jnp.where(li >= 2 * cy, cx + 2, 0)
            ya = i1 % cy + 2
            l2 = li - nxr
            xb = (l2 % (2 * cx)) // 2 + 2
            yb = l2 % 2 + jnp.where(l2 >= 2 * cx, cy + 2, 0)
            l3 = li - nxr - nyr
            xc = (l3 % 8) // 2 + jnp.where(l3 >= 16, cx + 2, -2)
            yc = l3 % 2 + jnp.where(l3 % 16 >= 8, cy + 2, 0)
            xe = jnp.where(l2 < 0, xa, jnp.where(l3 < 0, xb, xc))
            ye = jnp.where(l2 < 0, ya, jnp.where(l3 < 0, yb, yc))
            xe = jnp.where(l3 < 32, xe, -8)
            both = spread(served, xe, bx, 3) * spread(served, ye, by, 8)
            n = min(128, V.shape[1] - lo)
            hi, low = split(both)
            V[:, lo:lo + n], V_lo[:, lo:lo + n] = hi[:, 0:n], low[:, 0:n]
        li = lax.broadcasted_iota(jnp.int32, (1, 128), 1)
        ye = jnp.where(li < cy, li + 2, jnp.where(li < cy + 8, li - cy - 6, li - cy - 8 + cy + 2))
        ye = jnp.where(li < cy + 16, ye, -8)
        hi, lo = split(spread(served, ye, by, 8))
        k = cy + 16
        Wy[:, 0:k] = hi[:, 0:k]
        Wy[:, k:2 * k] = hi[:, 0:k]
        Wy[:, 2 * k:3 * k] = lo[:, 0:k]

    def build_z():
        served = served_table()
        bx, bz = corner(served, 0), corner(served, 2)
        wz_in[...] = spread(served, lane1 + 2, bz, 13)
        t = lane1 % 4
        tails = spread(served, jnp.where(t < 2, t, cz + t), bz, 13)
        for g in range(wzx.shape[0]):
            wzx[g] = tails * spread(served, lane1 // 16 + 2 + wide * (g - 1), bx, 3)

    def half(h, carry):
        m, sp, s, d = parts(h)
        hi, lo = split(T[m, pl.ds(s, 2), 2:2 + cx, y0:y1, :].reshape(2 * cx * cy, cz))
        DZ[...] = dot16(jnp.concatenate([hi, lo], axis=1), inner[...]).reshape(2, cx, cy, cz)
        recv_face(h, ZW)
        for g in range(cx // per):
            merged = jnp.where(tail < 2, zr[h, 0, g], zr[h, 1, g])
            l2, r2 = pltpu.roll(merged, cz - 2, 1), pltpu.roll(merged, 2, 1)
            l1, r1 = pltpu.roll(merged, cz - 1, 1), pltpu.roll(merged, 1, 1)
            fix = (jnp.where(tail < 2, -l2, r2)
                   + 8.0 * (jnp.where(tail == 1, l1, 0.0) - jnp.where(tail == 2, r1, 0.0)))
            for i in range(per):
                for q in range(2):
                    b = i * 8 + q * 4
                    DZ[q, g * per + i] = DZ[q, g * per + i] + jnp.where(
                        edge, pltpu.roll(fix, (2 * cz - b - 2) % cz, 1), 0.0)
        recv_face(h, YW)
        for q, c in enumerate((0, 2)):
            T[m, s + c, 2:2 + cx, y0 - 2:y0, :] = yr[h, 0, :, 2 * q:2 * q + 2, :]
            T[m, s + c, 2:2 + cx, y1:y1 + 2, :] = yr[h, 1, :, 2 * q:2 * q + 2, :]
        scale = step_size / (m + 1).astype(F32)
        plain = -scale / 12.0

        def plane(px):
            def d_x(c):
                at = lambda o: T[m, s + c, 2 + px + o, y0:y1, :]
                return (at(-2) - at(2)) + 8.0 * (at(1) - at(-1))

            def d_y(c):
                at = lambda o: T[m, s + c, 2 + px, y0 + o:y1 + o, :]
                return (at(-2) - at(2)) + 8.0 * (at(1) - at(-1))

            by = jnp.where(sp == 0, inv[px] * scale, plain)
            rates = ((d_y(2) - DZ[1, px]) * by, (DZ[0, px] - d_x(2)) * by, (d_x(1) - d_y(0)) * by)
            for c in range(3):
                T[m + 1, d + c, 2 + px, y0:y1, :] = rates[c]
                F[d + c, px] = F[d + c, px] + rates[c]

        for px in range(2, cx - 2):
            plane(px)
        recv_face(h, XW)
        for px in (0, 1, cx - 2, cx - 1):
            plane(px)

        @pl.when(h < 6)
        def _():
            start_face(h + 2, XW)
            pack_y(h + 2)
            start_face(h + 2, YW)
            pack_z(h + 2)
            start_face(h + 2, ZW)

        @pl.when(h >= 6)
        def _():
            send_final(h - 6)

        @pl.when(h == 3)
        def _():
            build_inner()

        @pl.when(h == 4)
        def _():
            build_outer()

        @pl.when(h == 5)
        def _():
            build_z()

        return carry

    lax.fori_loop(0, 8, half, 0)

    store = pltpu.make_async_copy(F, out, load_sem.at[6])
    store.start()

    depth = cx * cy

    def apply(w, w_lo, block):
        hi, lo = split(block)
        return dot16(w[...], hi) + dot16(w[...], lo) + dot16(w_lo[...], hi)

    for c in (3, 4, 5, 0, 1, 2):
        part[c] = apply(W, W_lo, F[c].reshape(depth, cz))

    slot_row = lax.broadcasted_iota(jnp.int32, (slots, cz), 0)
    slot_lane = lax.broadcasted_iota(jnp.int32, (slots, cz), 1)
    place = slot_row // served_rows * per_owner + slot_row % per_owner - slot_lane
    owner_of = slot_lane % 16 // 4
    result = jnp.zeros((slots, cz), F32)
    ktail = lax.broadcasted_iota(jnp.int32, (1, cz), 1) % 4 < 2
    for j in range(2):
        d = 3 * (1 - j)
        for way in [w for w in DIRS if w[2]] + [w for w in DIRS if not w[2]]:
            @pl.when(has[negate(way)])
            def _():
                final_copy(j, way).wait_recv()

        def ring(centre, low, high):
            return jnp.concatenate(
                [jnp.where(ktail, a[0], a[1]) for a in (centre, low, high)], axis=0)

        strips = [ring([ZX[j, 0, k] for k in range(2)], [ZXY[j, 0, 0, k] for k in range(2)],
                       [ZXY[j, 0, 1, k] for k in range(2)])]
        for g in range(cx // wide):
            strips.append(ring([ZR[j, k, g] for k in range(2)], [ZY[j, 0, k, g] for k in range(2)],
                               [ZY[j, 1, k, g] for k in range(2)]))
        strips.append(ring([ZX[j, 1, k] for k in range(2)], [ZXY[j, 1, 0, k] for k in range(2)],
                           [ZXY[j, 1, 1, k] for k in range(2)]))
        hi, lo = split(jnp.concatenate(strips, axis=1))
        zsum = dot16(Wy[...], jnp.concatenate([hi, lo, hi], axis=0))
        zpart = jnp.zeros((slots, cz), F32)
        for g in range(len(strips)):
            zpart = zpart + zsum[:, g * cz:(g + 1) * cz] * wzx[g]
        blocks = []
        for c in range(3):
            pieces = [XR[d + c].reshape(4 * cy, cz), YR[d + c].reshape(4 * cx, cz), XYR[d + c].reshape(32, cz)]
            blocks.append(jnp.concatenate(pieces, axis=0))
        added = apply(V, V_lo, jnp.concatenate(blocks, axis=1))
        for c in range(3):
            both = (part[d + c] + added[:, c * cz:(c + 1) * cz]) * wz_in[...]
            both = both + jnp.where(owner_of == c, zpart, 0.0)
            result = jnp.where(place == -(d + c) * cap, jnp.sum(both, axis=1, keepdims=True), result)

    folded = result[0:served_rows]
    for b in range(1, BLOCKS):
        folded = folded + result[b * served_rows:(b + 1) * served_rows]
    for o in range(group):
        ans[o] = jnp.sum(folded[o * per_owner:(o + 1) * per_owner], axis=0, keepdims=True)
    for d in range(1, group):
        answer(d).start()
    ansr[me] = ans[me]
    sel = lax.broadcasted_iota(jnp.int32, (8, 128), 1) // cap == lax.broadcasted_iota(jnp.int32, (8, 128), 0)
    wanted = lax.broadcasted_iota(jnp.int32, (rows, 128), 1) % cap == slot_s[...]
    for d in range(1, group):
        answer(d).wait_recv()
    got = jnp.concatenate([ansr[o] for o in range(group)], axis=0)
    picked = jnp.where(wanted, dot(hits_s[:, 0:group], got), 0.0)
    recept[...] = dot(sel.astype(F32), picked, ((1,), (1,)))[0:6]

    store.wait()

    def drain(h, carry):
        for way in FACES:
            @pl.when(has[way])
            def _():
                face_copy(h, way).wait_send()
        return carry

    lax.fori_loop(0, 8, drain, 0)
    for j in range(2):
        for way in DIRS:
            @pl.when(has[way])
            def _():
                final_copy(j, way).wait_send()
    for d in range(1, group):
        request(d).wait_send()
        answer(d).wait_send()


def local(sizes, fields, permittivity, donor_owner, donor_base, donor_weights):
    nx, ny, nz = sizes
    cx, cy, cz = permittivity.shape
    rows = donor_owner.shape[0]
    group = ny * nz
    cap = 2 * rows // group
    slots = group * cap
    per_owner = cap // BLOCKS
    vmem = pltpu.VMEM
    dma = pltpu.SemaphoreType.DMA
    yrows = cy + 16
    strips = cx * 8 // cz
    wide = cx * 16 // cz
    outer = 4 * cy + 4 * cx + 32
    out, recept = pl.pallas_call(
        functools.partial(kernel, (nx, ny, nz, cap)),
        out_shape=(
            jax.ShapeDtypeStruct(fields.shape, F32),
            jax.ShapeDtypeStruct((6, rows), F32),
        ),
        in_specs=[pl.BlockSpec(memory_space=pl.ANY)] * 5,
        out_specs=(pl.BlockSpec(memory_space=pl.ANY), pl.BlockSpec(memory_space=vmem)),
        scratch_shapes=[
            vmem((1, rows), jnp.int32),
            vmem((3, rows), jnp.int32),
            vmem((15, rows), F32),
            vmem((5, 6, cx + 4, yrows, cz), F32),
            vmem((6, cx, cy, cz), F32),
            vmem((cx, cy, cz), F32),
            vmem((8, 2, cx, 4, cz), F32),
            vmem((8, 2, cx, 4, cz), F32),
            vmem((8, strips, cy, cz), F32),
            vmem((8, 2, strips, cy, cz), F32),
            vmem((2, cx, cy, cz), F32),
            vmem((2, 2, 3, 2 * cx, cz), F32),
            vmem((2, wide, cy, cz), F32),
            vmem((6, 2, 2, cy, cz), F32),
            vmem((6, 2, 2 * cx, cz), F32),
            vmem((6, 2, 2, 8, cz), F32),
            vmem((2, 2, wide, cy, cz), F32),
            vmem((2, 2, 2, cy, cz), F32),
            vmem((2, 2, 2, wide, 8, cz), F32),
            vmem((2, 2, 2, 2, 8, cz), F32),
            vmem((128, rows), F32),
            vmem((2 * cz, cz), BF16),
            vmem((group, per_owner, 128), F32),
            vmem((group, per_owner, 128), F32),
            vmem((group, 1, 128), F32),
            vmem((group, 1, 128), F32),
            vmem((slots, cx * cy), BF16),
            vmem((slots, cx * cy), BF16),
            vmem((slots, outer), BF16),
            vmem((slots, outer), BF16),
            vmem((slots, 3 * (cy + 16)), BF16),
            vmem((wide + 2, slots, cz), F32),
            vmem((slots, cz), F32),
            vmem((rows, 128), F32),
            vmem((rows, 128), jnp.int32),
            vmem((6, slots, cz), F32),
            dma((8,)),
            dma((8, 6)),
            dma((8, 6)),
            dma((2, 26)),
            dma((2, 26)),
            dma((group,)),
            dma((group,)),
            dma((group,)),
            dma((group,)),
        ],
        compiler_params=pltpu.CompilerParams(
            collective_id=0, has_side_effects=True, vmem_limit_bytes=67043328
        ),
    )(fields, permittivity, donor_owner.T, donor_base.T, donor_weights.T)
    return out, recept


def solution(mesh):
    sizes = (mesh.shape["gx"], mesh.shape["gy"], mesh.shape["gz"])
    placed = (
        P(None, "gx", "gy", "gz"),
        P("gx", "gy", "gz"),
        P(("gx", "gy", "gz"), None),
        P(("gx", "gy", "gz"), None),
        P(("gx", "gy", "gz"), None),
    )
    return jax.shard_map(
        functools.partial(local, sizes),
        mesh=mesh,
        in_specs=placed,
        out_specs=(P(None, "gx", "gy", "gz"), P(None, ("gx", "gy", "gz"))),
        check_vma=False,
    )
```

```python
import functools

import jax
import jax.numpy as jnp
from jax import lax
from jax.experimental import pallas as pl
from jax.experimental.pallas import tpu as pltpu
from jax.sharding import PartitionSpec as P

step_size = 0.25
MESH = pl.DeviceIdType.MESH
F32 = jnp.float32
BF16 = jnp.bfloat16
HI = lax.Precision.HIGHEST
BLOCKS = 4
FEATURES = 32
DIRS = [(a, b, c) for a in (-1, 0, 1) for b in (-1, 0, 1) for c in (-1, 0, 1) if (a, b, c) != (0, 0, 0)]
FACES = [(-1, 0, 0), (1, 0, 0), (0, -1, 0), (0, 1, 0), (0, 0, -1), (0, 0, 1)]


def dot(a, b, dims=((1,), (0,))):
    return lax.dot_general(a, b, (dims, ((), ())), precision=HI, preferred_element_type=F32)


def split(a):
    hi = a.astype(BF16)
    return hi, (a - hi.astype(F32)).astype(BF16)


def dot16(a, b):
    return lax.dot_general(a, b, (((1,), (0,)), ((), ())), preferred_element_type=F32)


def negate(way):
    return tuple(-a for a in way)


def slot_of(a):
    return 0 if a < 0 else 1


def kernel(
    sizes, W_ring, fields, eps, owner_in, bases_in, weights_in, F, ansr, hits_t, slot_t,
    owner, bases, weights, T, inv, ys, yr, zs, zr, DZ,
    yfs, zfs, XR, YR, XYR, ZR, ZX, ZY, ZXY,
    data_t, inner, EX, EY, req, reqr, ans, W, W_lo, V, V_lo, Wy, wzx, wz_in, part,
    load_sem, send, recv, fsend, frecv, rsend, rrecv, asend, arecv,
):
    nx, ny, nz, cap = sizes
    group = ny * nz
    per_owner = cap // BLOCKS
    cx, cy, cz = eps.shape
    rows = owner.shape[1]
    slots = group * cap
    x, y, z = lax.axis_index("gx"), lax.axis_index("gy"), lax.axis_index("gz")
    me = y * nz + z
    y0, y1 = 8, 8 + cy

    loads = [
        pltpu.make_async_copy(fields, T.at[0, :, pl.ds(2, cx), pl.ds(8, cy), :], load_sem.at[0]),
        pltpu.make_async_copy(owner_in, owner, load_sem.at[1]),
        pltpu.make_async_copy(bases_in, bases, load_sem.at[2]),
        pltpu.make_async_copy(weights_in, weights, load_sem.at[3]),
        pltpu.make_async_copy(eps, inv, load_sem.at[4]),
        pltpu.make_async_copy(fields, F, load_sem.at[5]),
    ]
    for copy in loads:
        copy.start()

    has = {
        (-1, 0, 0): x > 0, (1, 0, 0): x < nx - 1, (0, -1, 0): y > 0,
        (0, 1, 0): y < ny - 1, (0, 0, -1): z > 0, (0, 0, 1): z < nz - 1,
    }
    for way in DIRS:
        found = None
        for axis in range(3):
            if way[axis]:
                face = tuple(way[a] if a == axis else 0 for a in range(3))
                found = has[face] if found is None else found & has[face]
        has[way] = found

    def dev(way):
        return (x + way[0], y + way[1], z + way[2])

    barrier = pltpu.get_barrier_semaphore()
    others = []
    for d in range(1, group):
        t = lax.rem(me + d, group)
        others.append((x, t // nz, lax.rem(t, nz)))
    expected = jnp.int32(group - 1)
    for way in DIRS:
        if way[0]:
            expected = expected + has[way].astype(jnp.int32)

            @pl.when(has[way])
            def _():
                pl.semaphore_signal(barrier, inc=1, device_id=dev(way), device_id_type=MESH)
    for target in others:
        pl.semaphore_signal(barrier, inc=1, device_id=target, device_id_type=MESH)

    lane = lax.broadcasted_iota(jnp.int32, (cy, cz), 1)
    lane1 = lax.broadcasted_iota(jnp.int32, (1, cz), 1)

    def remote(src, dst, s, r, target):
        return pltpu.make_async_remote_copy(
            src_ref=src, dst_ref=dst, send_sem=s, recv_sem=r, device_id=target, device_id_type=MESH)

    def request(d):
        return remote(req.at[(me + d) % group], reqr.at[me], rsend.at[d], rrecv.at[d], others[d - 1])

    def answer(d):
        return remote(ans.at[(me + d) % group], ansr.at[me], asend.at[d], arecv.at[d], others[d - 1])

    def parts(h):
        m = h // 2
        sp = (m + h % 2) % 2
        return m, sp, 3 * (1 - sp), 3 * sp

    def face_copy(h, way):
        m, sp, s, d = parts(h)
        i = FACES.index(way)
        if way[0]:
            lo_src, lo_dst = (2, cx + 2) if way[0] < 0 else (cx, 0)
            src = T.at[m, pl.ds(s + 1, 2), pl.ds(lo_src, 2), pl.ds(8, cy)]
            dst = T.at[m, pl.ds(s + 1, 2), pl.ds(lo_dst, 2), pl.ds(8, cy)]
        elif way[1]:
            k = slot_of(way[1])
            src, dst = ys.at[h, k], yr.at[h, 1 - k]
        else:
            src, dst = zs.at[h], zr.at[h, 1 - slot_of(way[2])]
        return remote(src, dst, send.at[h, i], recv.at[h, i], dev(way))

    def start_face(h, ways):
        for way in ways:
            @pl.when(has[way])
            def _():
                face_copy(h, way).start()

    def recv_face(h, ways):
        for way in ways:
            @pl.when(has[negate(way)])
            def _():
                face_copy(h, way).wait_recv()

    XW, YW, ZW = FACES[0:2], FACES[2:4], FACES[4:6]
    per = cz // 8

    def pack_y(h):
        m, sp, s, d = parts(h)
        for q, c in enumerate((0, 2)):
            ys[h, 0, :, 2 * q:2 * q + 2, :] = T[m, s + c, 2:2 + cx, y0:y0 + 2, :]
            ys[h, 1, :, 2 * q:2 * q + 2, :] = T[m, s + c, 2:2 + cx, y1 - 2:y1, :]

    def pack_z(h):
        m, sp, s, d = parts(h)
        for g in range(cx // per):
            strip = jnp.zeros((cy, cz), F32)
            for i in range(per):
                for q in range(2):
                    b = i * 8 + q * 4
                    strip = jnp.where(lane // 4 == b // 4,
                                      pltpu.roll(T[m, s + q, 2 + g * per + i, y0:y1, :], (b + 2) % cz, 1), strip)
            zs[h, g] = strip

    loads[0].wait()
    for h in range(2):
        pack_y(h)
        pack_z(h)
    pl.semaphore_wait(barrier, expected)
    for h in range(2):
        start_face(h, XW + YW + ZW)

    def clear(ref):
        ref[...] = jnp.zeros(ref.shape, F32)

    for way in DIRS:
        kx, ky, kz = (slot_of(a) for a in way)
        here = tuple(abs(a) for a in way)

        @pl.when(jnp.logical_not(has[way]))
        def _():
            if here == (1, 0, 0):
                for m in range(4):
                    clear(T.at[m, :, pl.ds(kx * (cx + 2), 2), pl.ds(8, cy)])
                clear(XR.at[:, kx])
            elif here == (0, 1, 0):
                clear(yr.at[:, ky])
                clear(YR.at[:, ky])
            elif here == (0, 0, 1):
                clear(zr.at[:, kz])
                clear(ZR.at[:, kz])
            elif here == (1, 1, 0):
                clear(XYR.at[:, kx, ky])
            elif here == (1, 0, 1):
                clear(ZX.at[:, kx, kz])
            elif here == (0, 1, 1):
                clear(ZY.at[:, ky, kz])
            else:
                clear(ZXY.at[:, kx, ky, kz])

    zi = lax.broadcasted_iota(jnp.int32, (2 * cz, cz), 0) % cz
    zo = lax.broadcasted_iota(jnp.int32, (2 * cz, cz), 1)
    delta = zi - zo
    inner[...] = (jnp.where(delta == -2, 1.0, 0.0) - jnp.where(delta == 2, 1.0, 0.0)
                  + jnp.where(delta == 1, 8.0, 0.0) - jnp.where(delta == -1, 8.0, 0.0)).astype(BF16)

    for copy in loads[1:4]:
        copy.wait()
    for b in range(BLOCKS):
        at = b * FEATURES
        data_t[at:at + 3] = bases[...].astype(F32)
        data_t[at + 3:at + 18] = weights[...]
        data_t[at + 18:at + FEATURES] = jnp.zeros((FEATURES - 18, rows), F32)
    own = owner[...]
    hits = jnp.where(lax.broadcasted_iota(jnp.int32, (group, rows), 0) == own, 1.0, 0.0)
    hits_t[...] = hits
    earlier = dot16(hits.astype(BF16), (lax.broadcasted_iota(jnp.int32, (rows, rows), 0)
                                        < lax.broadcasted_iota(jnp.int32, (rows, rows), 1)).astype(BF16))
    slot_f = jnp.sum(earlier * hits, axis=0, keepdims=True)
    slot_t[...] = slot_f
    slot = slot_f.astype(jnp.int32)
    block = lax.broadcasted_iota(jnp.int32, (BLOCKS * FEATURES, rows), 0) // FEATURES
    placed = jnp.where(block == slot // per_owner, data_t[...], 0.0)
    flat = own * per_owner + slot % per_owner
    perm = (flat == lax.broadcasted_iota(jnp.int32, (group * per_owner, rows), 0)).astype(F32)
    packed = dot(perm, placed, ((1,), (1,)))
    for o in range(group):
        req[o] = packed[o * per_owner:(o + 1) * per_owner]
    reqr[me] = req[me]
    for d in range(1, group):
        request(d).start()

    loads[4].wait()
    inv[...] = 1.0 / (12.0 * inv[...])
    loads[5].wait()
    here_x = lax.broadcasted_iota(jnp.int32, (64, 128), 0)
    inside = cx * cy
    ring_x, ring_y = 4 * cy, 4 * cx

    def one_hot(ref, lo, hot):
        hot = jnp.where(hot, 1.0, 0.0).astype(BF16)
        for k in range(3):
            ref[k * 64:(k + 1) * 64, lo:lo + 128] = hot
        ref[192:256, lo:lo + 128] = jnp.zeros((64, 128), BF16)

    def place(lo, xe, ye):
        one_hot(EX, lo, here_x == xe)
        one_hot(EY, lo, here_x - 32 == ye)

    for lo in range(0, inside, 128):
        li = lo + lane1
        place(lo, li // cy + 2, li % cy + 2)
    for lo in range(0, W_ring, 128):
        li = lo + lane1
        i1 = li % (2 * cy)
        l2 = li - ring_x
        l3 = li - ring_x - ring_y
        xe = jnp.where(
            l2 < 0, i1 // cy + jnp.where(li >= 2 * cy, cx + 2, 0),
            jnp.where(l3 < 0, (l2 % (2 * cx)) // 2 + 2, (l3 % 8) // 2 + jnp.where(l3 >= 16, cx + 2, -2)))
        ye = jnp.where(
            l2 < 0, i1 % cy + 2,
            jnp.where(l3 < 0, l2 % 2 + jnp.where(l2 >= 2 * cx, cy + 2, 0),
                      l3 % 2 + jnp.where(l3 % 16 >= 8, cy + 2, 0)))
        place(inside + lo, jnp.where((l3 < 32) & (xe < 32), xe, -100), jnp.where(l3 < 32, ye, -100))
    ye = jnp.where(lane1 < cy, lane1 + 2, jnp.where(lane1 < cy + 8, lane1 - cy - 6, lane1 - 6))
    one_hot(EY, inside + W_ring, here_x - 32 == jnp.where(lane1 < cy + 16, ye, -100))
    wide = cz // 16
    for g in range(wzx.shape[0]):
        xe = lane1 // 16 + 2 + wide * (g - 1)
        one_hot(EX, inside + W_ring + 128 * g, here_x == jnp.where(xe < 32, xe, -100))

    edge = (lane < 2) | (lane >= cz - 2)
    tail = lane % 4

    def final_copy(j, way):
        i = DIRS.index(way)
        d = 3 * (1 - j)
        here = tuple(abs(a) for a in way)
        kx, ky, kz = (slot_of(a) for a in way)
        nx_, ny_, nz_ = 1 - kx, 1 - ky, 1 - kz
        strip = kx * (zfs.shape[1] - 1)
        if here == (1, 0, 0):
            src, dst = F.at[pl.ds(d, 3), pl.ds(kx * (cx - 2), 2)], XR.at[pl.ds(d, 3), nx_]
        elif here == (0, 1, 0):
            src, dst = yfs.at[j, ky], YR.at[pl.ds(d, 3), ny_]
        elif here == (0, 0, 1):
            src, dst = zfs.at[j], ZR.at[j, nz_]
        elif here == (1, 1, 0):
            src = yfs.at[j, ky, :, pl.ds(kx * (2 * cx - 8), 8)]
            dst = XYR.at[pl.ds(d, 3), nx_, ny_]
        elif here == (1, 0, 1):
            src, dst = zfs.at[j, strip], ZX.at[j, nx_, nz_]
        elif here == (0, 1, 1):
            src, dst = zfs.at[j, :, pl.ds(ky * (cy - 8), 8)], ZY.at[j, ny_, nz_]
        else:
            src, dst = zfs.at[j, strip, pl.ds(ky * (cy - 8), 8)], ZXY.at[j, nx_, ny_, nz_]
        return remote(src, dst, fsend.at[j, i], frecv.at[j, i], dev(way))

    def start_final(j, ways):
        for way in ways:
            @pl.when(has[way])
            def _():
                final_copy(j, way).start()

    def send_final(j):
        d = 3 * (1 - j)
        start_final(j, XW)
        for g in range(cx // wide):
            strip = jnp.zeros((cy, cz), F32)
            for i in range(wide):
                for c in range(3):
                    b = i * 16 + c * 4
                    strip = jnp.where(lane // 4 == b // 4,
                                      pltpu.roll(F[d + c, g * wide + i], (b + 2) % cz, 1), strip)
            zfs[j, g] = strip
        start_final(j, sorted((way for way in DIRS if way[2]), key=lambda way: -sum(map(abs, way))))
        for k, lo in ((0, 0), (1, cy - 2)):
            for c in range(3):
                for px in range(cx):
                    yfs[j, k, c, 2 * px:2 * px + 2, :] = F[d + c, px, lo:lo + 2, :]
        start_final(j, [way for way in DIRS if way[0] and way[1] and not way[2]] + YW)

    served_rows = group * per_owner

    def served_table():
        if per_owner % 8 == 0:
            table = reqr[...].reshape(served_rows, 128)
        else:
            table = jnp.concatenate([reqr[o] for o in range(group)], axis=0)
        turned = [table] + [pltpu.roll(table, 128 - b * FEATURES, 1) for b in range(1, BLOCKS)]
        return jnp.concatenate(turned, axis=0)

    def build():
        for d in range(1, group):
            request(d).wait_recv()
        served = served_table()

        def column(k):
            return jnp.broadcast_to(served[:, k:k + 1], (slots, 128))

        li = lax.broadcasted_iota(jnp.int32, (slots, 128), 1)
        flat_lane = li.astype(F32)
        bx, by, bz = column(0), column(1), column(2)
        in_x, in_xy = li < 32, li < 64
        off = jnp.where(in_x, flat_lane - bx, flat_lane - 32.0 - by)
        t = li % 4
        off_z = flat_lane + 2.0 - bz
        off_t = jnp.where(t < 2, t, cz + t).astype(F32) - bz
        both = jnp.zeros((slots, 128), F32)
        z_in = jnp.zeros((slots, 128), F32)
        tails = jnp.zeros((slots, 128), F32)
        for k in range(5):
            wz = column(13 + k)
            both = jnp.where(off == k, jnp.where(in_x, column(3 + k), column(8 + k)), both)
            z_in = jnp.where(off_z == k, wz, z_in)
            tails = jnp.where(off_t == k, wz, tails)
        wz_in[...] = z_in
        both = jnp.where(in_xy, both, 0.0)
        hi = both.astype(BF16).astype(F32)
        mid = (both - hi).astype(BF16).astype(F32)
        table = jnp.concatenate([(hi + pltpu.roll(mid, 64, 1)).astype(BF16), (both - hi - mid).astype(BF16)], axis=1)

        def weights_at(lo, n):
            return dot16(table, EX[:, lo:lo + n]) * dot16(table, EY[:, lo:lo + n])

        W[...], W_lo[...] = split(weights_at(0, inside))
        n = V.shape[1]
        hi, lo = split(weights_at(inside, W_ring))
        V[...], V_lo[...] = hi[:, 0:n], lo[:, 0:n]
        k = cy + 16
        hi, lo = split(dot16(table, EY[:, inside + W_ring:inside + W_ring + 128]))
        Wy[:, 0:k] = hi[:, 0:k]
        Wy[:, k:2 * k] = hi[:, 0:k]
        Wy[:, 2 * k:3 * k] = lo[:, 0:k]
        at_x = dot16(table, EX[:, inside + W_ring:])
        for g in range(wzx.shape[0]):
            wzx[g] = tails * at_x[:, g * 128:(g + 1) * 128]

    def half(h, carry):
        m, sp, s, d = parts(h)
        hi, lo = split(T[m, pl.ds(s, 2), 2:2 + cx, y0:y1, :].reshape(2 * cx * cy, cz))
        DZ[...] = dot16(jnp.concatenate([hi, lo], axis=1), inner[...]).reshape(2, cx, cy, cz)
        @pl.when(h == 4)
        def _():
            build()

        recv_face(h, ZW)
        for g in range(cx // per):
            merged = jnp.where(tail < 2, zr[h, 0, g], zr[h, 1, g])
            l2, r2 = pltpu.roll(merged, cz - 2, 1), pltpu.roll(merged, 2, 1)
            l1, r1 = pltpu.roll(merged, cz - 1, 1), pltpu.roll(merged, 1, 1)
            fix = (jnp.where(tail < 2, -l2, r2)
                   + 8.0 * (jnp.where(tail == 1, l1, 0.0) - jnp.where(tail == 2, r1, 0.0)))
            for i in range(per):
                for q in range(2):
                    b = i * 8 + q * 4
                    DZ[q, g * per + i] = DZ[q, g * per + i] + jnp.where(
                        edge, pltpu.roll(fix, (2 * cz - b - 2) % cz, 1), 0.0)
        recv_face(h, YW)
        for q, c in enumerate((0, 2)):
            T[m, s + c, 2:2 + cx, y0 - 2:y0, :] = yr[h, 0, :, 2 * q:2 * q + 2, :]
            T[m, s + c, 2:2 + cx, y1:y1 + 2, :] = yr[h, 1, :, 2 * q:2 * q + 2, :]
        scale = step_size / (m + 1).astype(F32)
        plain = -scale / 12.0

        def plane(px):
            def d_x(c):
                at = lambda o: T[m, s + c, 2 + px + o, y0:y1, :]
                return (at(-2) - at(2)) + 8.0 * (at(1) - at(-1))

            def d_y(c):
                at = lambda o: T[m, s + c, 2 + px, y0 + o:y1 + o, :]
                return (at(-2) - at(2)) + 8.0 * (at(1) - at(-1))

            by = jnp.where(sp == 0, inv[px] * scale, plain)
            rates = ((d_y(2) - DZ[1, px]) * by, (DZ[0, px] - d_x(2)) * by, (d_x(1) - d_y(0)) * by)
            for c in range(3):
                T[m + 1, d + c, 2 + px, y0:y1, :] = rates[c]
                F[d + c, px] = F[d + c, px] + rates[c]

        for px in range(2, cx - 2):
            plane(px)
        recv_face(h, XW)
        for px in (0, 1, cx - 2, cx - 1):
            plane(px)

        @pl.when(h < 6)
        def _():
            start_face(h + 2, XW)
            pack_y(h + 2)
            start_face(h + 2, YW)
            pack_z(h + 2)
            start_face(h + 2, ZW)

        @pl.when(h >= 6)
        def _():
            send_final(h - 6)

        return carry

    lax.fori_loop(0, 8, half, 0)

    depth = cx * cy

    def apply(w, w_lo, block):
        hi, lo = split(block)
        return dot16(w[...], hi) + dot16(w[...], lo) + dot16(w_lo[...], hi)

    for c in (3, 4, 5, 0, 1, 2):
        part[c] = apply(W, W_lo, F[c].reshape(depth, cz))

    slot_row = lax.broadcasted_iota(jnp.int32, (slots, cz), 0)
    slot_lane = lax.broadcasted_iota(jnp.int32, (slots, cz), 1)
    target = slot_row // served_rows * per_owner + slot_row % per_owner - slot_lane
    owner_of = slot_lane % 16 // 4
    result = jnp.zeros((slots, cz), F32)
    ktail = lax.broadcasted_iota(jnp.int32, (1, cz), 1) % 4 < 2
    for j in range(2):
        d = 3 * (1 - j)
        for way in [w for w in DIRS if w[2]] + [w for w in DIRS if not w[2]]:
            @pl.when(has[negate(way)])
            def _():
                final_copy(j, way).wait_recv()

        def ring(centre, low, high):
            return jnp.concatenate(
                [jnp.where(ktail, a[0], a[1]) for a in (centre, low, high)], axis=0)

        strips = [ring([ZX[j, 0, k] for k in range(2)], [ZXY[j, 0, 0, k] for k in range(2)],
                       [ZXY[j, 0, 1, k] for k in range(2)])]
        for g in range(cx // wide):
            strips.append(ring([ZR[j, k, g] for k in range(2)], [ZY[j, 0, k, g] for k in range(2)],
                               [ZY[j, 1, k, g] for k in range(2)]))
        strips.append(ring([ZX[j, 1, k] for k in range(2)], [ZXY[j, 1, 0, k] for k in range(2)],
                           [ZXY[j, 1, 1, k] for k in range(2)]))
        hi, lo = split(jnp.concatenate(strips, axis=1))
        zsum = dot16(Wy[...], jnp.concatenate([hi, lo, hi], axis=0))
        zpart = jnp.zeros((slots, cz), F32)
        for g in range(len(strips)):
            zpart = zpart + zsum[:, g * cz:(g + 1) * cz] * wzx[g]
        blocks = []
        for c in range(3):
            pieces = [XR[d + c].reshape(4 * cy, cz), YR[d + c].reshape(4 * cx, cz), XYR[d + c].reshape(32, cz)]
            blocks.append(jnp.concatenate(pieces, axis=0))
        added = apply(V, V_lo, jnp.concatenate(blocks, axis=1))
        for c in range(3):
            both = (part[d + c] + added[:, c * cz:(c + 1) * cz]) * wz_in[...]
            both = both + jnp.where(owner_of == c, zpart, 0.0)
            result = jnp.where(target == -(d + c) * cap, jnp.sum(both, axis=1, keepdims=True), result)

    folded = result[0:served_rows]
    for b in range(1, BLOCKS):
        folded = folded + result[b * served_rows:(b + 1) * served_rows]
    for o in range(group):
        ans[o] = jnp.sum(folded[o * per_owner:(o + 1) * per_owner], axis=0, keepdims=True)
    for d in range(1, group):
        answer(d).start()
    ansr[me] = ans[me]

    def drain(h, carry):
        for way in FACES:
            @pl.when(has[way])
            def _():
                face_copy(h, way).wait_send()
        return carry

    lax.fori_loop(0, 8, drain, 0)
    for j in range(2):
        for way in DIRS:
            @pl.when(has[way])
            def _():
                final_copy(j, way).wait_send()
    for d in range(1, group):
        request(d).wait_send()
    for d in range(1, group):
        answer(d).wait_recv()
    for d in range(1, group):
        answer(d).wait_send()


def finish_kernel(cap, F, ansr, hits_t, slot_t, out, recept, sem):
    store = pltpu.make_async_copy(F, out, sem.at[0])
    store.start()
    group = ansr.shape[0]
    got = jnp.concatenate([ansr[o] for o in range(group)], axis=0)
    hi, low = split(got)
    mid, lo = split(got - hi.astype(F32))
    hits = hits_t[...].astype(BF16)
    picked = lax.dot_general(jnp.concatenate([hi, mid, lo], axis=0), jnp.concatenate([hits] * 3, axis=0),
                             (((0,), (0,)), ((), ())), preferred_element_type=F32)
    at = lax.broadcasted_iota(jnp.int32, picked.shape, 0) % cap
    picked = jnp.where(at == slot_t[...].astype(jnp.int32), picked, 0.0)
    for c in range(6):
        recept[c:c + 1] = jnp.sum(picked[c * cap:(c + 1) * cap], axis=0, keepdims=True)
    store.wait()


def local(sizes, fields, permittivity, donor_owner, donor_base, donor_weights):
    nx, ny, nz = sizes
    cx, cy, cz = permittivity.shape
    rows = donor_owner.shape[0]
    group = ny * nz
    cap = 2 * rows // group
    slots = group * cap
    per_owner = cap // BLOCKS
    vmem = pltpu.VMEM
    dma = pltpu.SemaphoreType.DMA
    yrows = cy + 16
    strips = cx * 8 // cz
    wide = cx * 16 // cz
    outer = 4 * cy + 4 * cx + 32
    ring = -(-outer // 128) * 128
    new, *answers = pl.pallas_call(
        functools.partial(kernel, (nx, ny, nz, cap), ring),
        out_shape=(
            vmem(fields.shape, F32),
            vmem((group, 1, 128), F32),
            vmem((group, rows), F32),
            vmem((1, rows), F32),
        ),
        in_specs=[pl.BlockSpec(memory_space=pl.ANY)] * 5,
        out_specs=(pl.BlockSpec(memory_space=vmem),) * 4,
        scratch_shapes=[
            vmem((1, rows), jnp.int32),
            vmem((3, rows), jnp.int32),
            vmem((15, rows), F32),
            vmem((5, 6, cx + 4, yrows, cz), F32),
            vmem((cx, cy, cz), F32),
            vmem((8, 2, cx, 4, cz), F32),
            vmem((8, 2, cx, 4, cz), F32),
            vmem((8, strips, cy, cz), F32),
            vmem((8, 2, strips, cy, cz), F32),
            vmem((2, cx, cy, cz), F32),
            vmem((2, 2, 3, 2 * cx, cz), F32),
            vmem((2, wide, cy, cz), F32),
            vmem((6, 2, 2, cy, cz), F32),
            vmem((6, 2, 2 * cx, cz), F32),
            vmem((6, 2, 2, 8, cz), F32),
            vmem((2, 2, wide, cy, cz), F32),
            vmem((2, 2, 2, cy, cz), F32),
            vmem((2, 2, 2, wide, 8, cz), F32),
            vmem((2, 2, 2, 2, 8, cz), F32),
            vmem((128, rows), F32),
            vmem((2 * cz, cz), BF16),
            vmem((256, cx * cy + ring + 128 * (wide + 2)), BF16),
            vmem((256, cx * cy + ring + 128), BF16),
            vmem((group, per_owner, 128), F32),
            vmem((group, per_owner, 128), F32),
            vmem((group, 1, 128), F32),
            vmem((slots, cx * cy), BF16),
            vmem((slots, cx * cy), BF16),
            vmem((slots, outer), BF16),
            vmem((slots, outer), BF16),
            vmem((slots, 3 * (cy + 16)), BF16),
            vmem((wide + 2, slots, cz), F32),
            vmem((slots, cz), F32),
            vmem((6, slots, cz), F32),
            dma((8,)),
            dma((8, 6)),
            dma((8, 6)),
            dma((2, 26)),
            dma((2, 26)),
            dma((group,)),
            dma((group,)),
            dma((group,)),
            dma((group,)),
        ],
        compiler_params=pltpu.CompilerParams(
            collective_id=0, has_side_effects=True, vmem_limit_bytes=60 * 1024 * 1024
        ),
    )(fields, permittivity, donor_owner.T, donor_base.T, donor_weights.T)
    return pl.pallas_call(
        functools.partial(finish_kernel, cap),
        out_shape=(
            jax.ShapeDtypeStruct(fields.shape, F32),
            jax.ShapeDtypeStruct((6, rows), F32),
        ),
        in_specs=[pl.BlockSpec(memory_space=vmem)] * 4,
        out_specs=(pl.BlockSpec(memory_space=pl.ANY), pl.BlockSpec(memory_space=vmem)),
        scratch_shapes=[dma((1,))],
        compiler_params=pltpu.CompilerParams(vmem_limit_bytes=2 * 1024 * 1024),
    )(new, *answers)


def solution(mesh):
    sizes = (mesh.shape["gx"], mesh.shape["gy"], mesh.shape["gz"])
    placed = (
        P(None, "gx", "gy", "gz"),
        P("gx", "gy", "gz"),
        P(("gx", "gy", "gz"), None),
        P(("gx", "gy", "gz"), None),
        P(("gx", "gy", "gz"), None),
    )
    return jax.shard_map(
        functools.partial(local, sizes),
        mesh=mesh,
        in_specs=placed,
        out_specs=(P(None, "gx", "gy", "gz"), P(None, ("gx", "gy", "gz"))),
        check_vma=False,
    )
```

```python
import functools

import jax
import jax.numpy as jnp
from jax import lax
from jax.experimental import pallas as pl
from jax.experimental.pallas import tpu as pltpu
from jax.sharding import PartitionSpec as P

step_size = 0.25
MESH = pl.DeviceIdType.MESH
F32 = jnp.float32
BF16 = jnp.bfloat16
HI = lax.Precision.HIGHEST
BLOCKS = 4
FEATURES = 32
DIRS = [(a, b, c) for a in (-1, 0, 1) for b in (-1, 0, 1) for c in (-1, 0, 1) if (a, b, c) != (0, 0, 0)]
FACES = [(-1, 0, 0), (1, 0, 0), (0, -1, 0), (0, 1, 0), (0, 0, -1), (0, 0, 1)]


def dot(a, b, dims=((1,), (0,))):
    return lax.dot_general(a, b, (dims, ((), ())), precision=HI, preferred_element_type=F32)


def split(a):
    hi = a.astype(BF16)
    return hi, (a - hi.astype(F32)).astype(BF16)


def dot16(a, b):
    return lax.dot_general(a, b, (((1,), (0,)), ((), ())), preferred_element_type=F32)


def negate(way):
    return tuple(-a for a in way)


def slot_of(a):
    return 0 if a < 0 else 1


def kernel(
    sizes, W_ring, fields, eps, owner_in, bases_in, weights_in, F, ansr, hits_t, slot_t,
    owner, bases, weights, T, inv, ys, yr, zs, zr, DZ,
    yfs, zfs, zys, XR, YR, XYR, ZR, ZX, ZY, ZXY,
    data_t, inner, gather, EX, EY, req, reqr, ans, W, W_lo, V, V_lo, Wy, wzx, wz_in, part,
    z_sem, y_sem, load_sem, send, recv, fsend, frecv, rsend, rrecv, asend, arecv,
):
    nx, ny, nz, cap = sizes
    group = ny * nz
    per_owner = cap // BLOCKS
    cx, cy, cz = eps.shape
    rows = owner.shape[1]
    slots = group * cap
    x, y, z = lax.axis_index("gx"), lax.axis_index("gy"), lax.axis_index("gz")
    me = y * nz + z
    y0, y1 = 8, 8 + cy

    loads = [
        pltpu.make_async_copy(fields, T.at[0, :, pl.ds(2, cx), pl.ds(8, cy), :], load_sem.at[0]),
        pltpu.make_async_copy(owner_in, owner, load_sem.at[1]),
        pltpu.make_async_copy(bases_in, bases, load_sem.at[2]),
        pltpu.make_async_copy(weights_in, weights, load_sem.at[3]),
        pltpu.make_async_copy(eps, inv, load_sem.at[4]),
        pltpu.make_async_copy(fields, F, load_sem.at[5]),
    ]
    for copy in loads[0:5]:
        copy.start()

    has = {
        (-1, 0, 0): x > 0, (1, 0, 0): x < nx - 1, (0, -1, 0): y > 0,
        (0, 1, 0): y < ny - 1, (0, 0, -1): z > 0, (0, 0, 1): z < nz - 1,
    }
    for way in DIRS:
        found = None
        for axis in range(3):
            if way[axis]:
                face = tuple(way[a] if a == axis else 0 for a in range(3))
                found = has[face] if found is None else found & has[face]
        has[way] = found

    def dev(way):
        return (x + way[0], y + way[1], z + way[2])

    barrier = pltpu.get_barrier_semaphore()
    others = []
    for d in range(1, group):
        t = lax.rem(me + d, group)
        others.append((x, t // nz, lax.rem(t, nz)))
    expected = jnp.int32(0)
    for way in FACES:
        expected = expected + has[way].astype(jnp.int32)

        @pl.when(has[way])
        def _():
            pl.semaphore_signal(barrier, inc=1, device_id=dev(way), device_id_type=MESH)

    def line_stage(k, at, count, sems, up):
        down = negate(up)
        for here, side, way in ((at == k, 0, up), (at == count - 1 - k, 1, down)):
            @pl.when(here)
            def _():
                if k > 0:
                    pl.semaphore_wait(sems.at[side], 1)
                if k < count - 1:
                    pl.semaphore_signal(sems.at[side], inc=1, device_id=dev(way), device_id_type=MESH)

    def z_stage(k):
        line_stage(k, z, nz, z_sem, (0, 0, 1))

    def y_stage(k):
        line_stage(k, y, ny, y_sem, (0, 1, 0))

    lane = lax.broadcasted_iota(jnp.int32, (cy, cz), 1)
    lane1 = lax.broadcasted_iota(jnp.int32, (1, cz), 1)

    def remote(src, dst, s, r, target):
        return pltpu.make_async_remote_copy(
            src_ref=src, dst_ref=dst, send_sem=s, recv_sem=r, device_id=target, device_id_type=MESH)

    def request(d):
        return remote(req.at[(me + d) % group], reqr.at[me], rsend.at[d], rrecv.at[d], others[d - 1])

    def answer(d):
        return remote(ans.at[(me + d) % group], ansr.at[me], asend.at[d], arecv.at[d], others[d - 1])

    def parts(h):
        m = h // 2
        sp = (m + h % 2) % 2
        return m, sp, 3 * (1 - sp), 3 * sp

    def face_copy(h, way):
        m, sp, s, d = parts(h)
        i = FACES.index(way)
        if way[0]:
            lo_src, lo_dst = (2, cx + 2) if way[0] < 0 else (cx, 0)
            src = T.at[m, pl.ds(s + 1, 2), pl.ds(lo_src, 2), pl.ds(8, cy)]
            dst = T.at[m, pl.ds(s + 1, 2), pl.ds(lo_dst, 2), pl.ds(8, cy)]
        elif way[1]:
            k = slot_of(way[1])
            src, dst = ys.at[h, k], yr.at[h, 1 - k]
        else:
            src, dst = zs.at[h], zr.at[h, 1 - slot_of(way[2])]
        return remote(src, dst, send.at[h, i], recv.at[h, i], dev(way))

    def start_face(h, ways):
        for way in ways:
            @pl.when(has[way])
            def _():
                face_copy(h, way).start()

    def recv_face(h, ways):
        for way in ways:
            @pl.when(has[negate(way)])
            def _():
                face_copy(h, way).wait_recv()

    XW, YW, ZW = FACES[0:2], FACES[2:4], FACES[4:6]
    per = cz // 8

    def pack_y(h):
        m, sp, s, d = parts(h)
        for q, c in enumerate((0, 2)):
            ys[h, 0, :, 2 * q:2 * q + 2, :] = T[m, s + c, 2:2 + cx, y0:y0 + 2, :]
            ys[h, 1, :, 2 * q:2 * q + 2, :] = T[m, s + c, 2:2 + cx, y1 - 2:y1, :]

    def pack_z(h):
        m, sp, s, d = parts(h)
        for g in range(cx // per):
            strip = jnp.zeros((cy, cz), F32)
            for i in range(per):
                for q in range(2):
                    b = i * 8 + q * 4
                    strip = jnp.where(lane // 4 == b // 4,
                                      pltpu.roll(T[m, s + q, 2 + g * per + i, y0:y1, :], (b + 2) % cz, 1), strip)
            zs[h, g] = strip

    loads[0].wait()
    loads[5].start()
    for h in range(2):
        pack_y(h)
    pl.semaphore_wait(barrier, expected)
    for h in range(2):
        start_face(h, YW + XW)
        pack_z(h)
        start_face(h, ZW)
    z_stage(0)

    def clear(ref):
        ref[...] = jnp.zeros(ref.shape, F32)

    for way in DIRS:
        kx, ky, kz = (slot_of(a) for a in way)
        here = tuple(abs(a) for a in way)

        @pl.when(jnp.logical_not(has[way]))
        def _():
            if here == (1, 0, 0):
                for m in range(4):
                    clear(T.at[m, :, pl.ds(kx * (cx + 2), 2), pl.ds(8, cy)])
                clear(XR.at[:, kx])
            elif here == (0, 1, 0):
                clear(yr.at[:, ky])
                clear(YR.at[:, ky])
            elif here == (0, 0, 1):
                clear(zr.at[:, kz])
                clear(ZR.at[kz])
            elif here == (1, 1, 0):
                clear(XYR.at[:, kx, ky])
            elif here == (1, 0, 1):
                clear(ZX.at[kx, kz])
            elif here == (0, 1, 1):
                clear(ZY.at[ky, kz])
            else:
                clear(ZXY.at[kx, ky, kz])

    zi = lax.broadcasted_iota(jnp.int32, (2 * cz, cz), 0) % cz
    zo = lax.broadcasted_iota(jnp.int32, (2 * cz, cz), 1)
    delta = zi - zo
    inner[...] = (jnp.where(delta == -2, 1.0, 0.0) - jnp.where(delta == 2, 1.0, 0.0)
                  + jnp.where(delta == 1, 8.0, 0.0) - jnp.where(delta == -1, 8.0, 0.0)).astype(BF16)

    for copy in loads[1:4]:
        copy.wait()
    for b in range(BLOCKS):
        at = b * FEATURES
        data_t[at:at + 3] = bases[...].astype(F32)
        data_t[at + 3:at + 18] = weights[...]
        data_t[at + 18:at + FEATURES] = jnp.zeros((FEATURES - 18, rows), F32)
    own = owner[...]
    hits = jnp.where(lax.broadcasted_iota(jnp.int32, (group, rows), 0) == own, 1.0, 0.0)
    hits_t[...] = hits
    earlier = dot16(hits.astype(BF16), (lax.broadcasted_iota(jnp.int32, (rows, rows), 0)
                                        < lax.broadcasted_iota(jnp.int32, (rows, rows), 1)).astype(BF16))
    slot_f = jnp.sum(earlier * hits, axis=0, keepdims=True)
    slot_t[...] = slot_f
    slot = slot_f.astype(jnp.int32)
    block = lax.broadcasted_iota(jnp.int32, (BLOCKS * FEATURES, rows), 0) // FEATURES
    placed = jnp.where(block == slot // per_owner, data_t[...], 0.0)
    flat = own * per_owner + slot % per_owner
    perm = (flat == lax.broadcasted_iota(jnp.int32, (group * per_owner, rows), 0)).astype(F32)
    packed = dot(perm, placed, ((1,), (1,)))
    for o in range(group):
        req[o] = packed[o * per_owner:(o + 1) * per_owner]
    reqr[me] = req[me]
    loads[4].wait()
    inv[...] = 1.0 / (12.0 * inv[...])
    loads[5].wait()
    here_x = lax.broadcasted_iota(jnp.int32, (64, 128), 0)
    inside = cx * cy
    ring_x, ring_y = 4 * cy, 4 * cx

    def one_hot(ref, lo, hot):
        hot = jnp.where(hot, 1.0, 0.0).astype(BF16)
        for k in range(3):
            ref[k * 64:(k + 1) * 64, lo:lo + 128] = hot
        ref[192:256, lo:lo + 128] = jnp.zeros((64, 128), BF16)

    def place(lo, xe, ye):
        one_hot(EX, lo, here_x == xe)
        one_hot(EY, lo, here_x - 32 == ye)

    for lo in range(0, inside, 128):
        li = lo + lane1
        place(lo, li // cy + 2, li % cy + 2)
    for lo in range(0, W_ring, 128):
        li = lo + lane1
        i1 = li % (2 * cy)
        l2 = li - ring_x
        l3 = li - ring_x - ring_y
        xe = jnp.where(
            l2 < 0, i1 // cy + jnp.where(li >= 2 * cy, cx + 2, 0),
            jnp.where(l3 < 0, (l2 % (2 * cx)) // 2 + 2, (l3 % 4) // 2 + jnp.where(l3 >= 8, cx + 2, 0)))
        ye = jnp.where(
            l2 < 0, i1 % cy + 2,
            jnp.where(l3 < 0, l2 % 2 + jnp.where(l2 >= 2 * cx, cy + 2, 0),
                      l3 % 2 + jnp.where(l3 % 8 >= 4, cy + 2, 0)))
        place(inside + lo, jnp.where(l3 < 16, xe, -100), jnp.where(l3 < 16, ye, -100))
    ye = jnp.where(lane1 < cy, lane1 + 2, jnp.where(lane1 < cy + 2, lane1 - cy, lane1))
    one_hot(EY, inside + W_ring, here_x - 32 == jnp.where(lane1 < cy + 4, ye, -100))
    wide = cz // 32
    for g in range(wzx.shape[0]):
        xe = lane1 // 32 + 2 + wide * (g - 1)
        one_hot(EX, inside + W_ring + 128 * g, here_x == jnp.where(xe < 32, xe, -100))
    comp_row = lax.broadcasted_iota(jnp.int32, (2 * cz, cz), 0) % 32 // 4
    comp_col = lax.broadcasted_iota(jnp.int32, (2 * cz, cz), 1) // cap
    gather[...] = jnp.where((comp_row == comp_col) & (comp_row < 6), 1.0, 0.0).astype(BF16)
    for k in range(1, min(2, nz)):
        z_stage(k)

    edge = (lane < 2) | (lane >= cz - 2)
    tail = lane % 4

    def final_copy(j, way):
        i = DIRS.index(way)
        d = 3 * (1 - j)
        here = tuple(abs(a) for a in way)
        kx, ky, kz = (slot_of(a) for a in way)
        nx_, ny_, nz_ = 1 - kx, 1 - ky, 1 - kz
        strip = kx * (zfs.shape[0] - 1)
        if here == (1, 0, 0):
            src, dst = F.at[pl.ds(d, 3), pl.ds(kx * (cx - 2), 2)], XR.at[pl.ds(d, 3), nx_]
        elif here == (0, 1, 0):
            src, dst = yfs.at[j, ky], YR.at[pl.ds(d, 3), ny_]
        elif here == (0, 0, 1):
            src, dst = zfs, ZR.at[nz_]
        elif here == (1, 1, 0):
            src = yfs.at[j, ky, :, kx * (cx // 2 - 1)]
            dst = XYR.at[pl.ds(d, 3), nx_, ny_]
        elif here == (1, 0, 1):
            src, dst = zfs.at[strip], ZX.at[nx_, nz_]
        elif here == (0, 1, 1):
            src, dst = zys.at[ky], ZY.at[ny_, nz_]
        else:
            src, dst = zys.at[ky, strip], ZXY.at[nx_, ny_, nz_]
        return remote(src, dst, fsend.at[j, i], frecv.at[j, i], dev(way))

    def start_final(j, ways):
        for way in ways:
            @pl.when(has[way])
            def _():
                final_copy(j, way).start()

    served_rows = group * per_owner

    def served_table():
        if per_owner % 8 == 0:
            table = reqr[...].reshape(served_rows, 128)
        else:
            table = jnp.concatenate([reqr[o] for o in range(group)], axis=0)
        turned = [table] + [pltpu.roll(table, 128 - b * FEATURES, 1) for b in range(1, BLOCKS)]
        return jnp.concatenate(turned, axis=0)

    def build():
        for d in range(1, group):
            request(d).wait_recv()
        served = served_table()

        def column(k):
            return jnp.broadcast_to(served[:, k:k + 1], (slots, 128))

        li = lax.broadcasted_iota(jnp.int32, (slots, 128), 1)
        flat_lane = li.astype(F32)
        bx, by, bz = column(0), column(1), column(2)
        in_x, in_xy = li < 32, li < 64
        off = jnp.where(in_x, flat_lane - bx, flat_lane - 32.0 - by)
        t = li % 4
        off_z = flat_lane + 2.0 - bz
        off_t = jnp.where(t < 2, t, cz + t).astype(F32) - bz
        both = jnp.zeros((slots, 128), F32)
        z_in = jnp.zeros((slots, 128), F32)
        tails = jnp.zeros((slots, 128), F32)
        for k in range(5):
            wz = column(13 + k)
            both = jnp.where(off == k, jnp.where(in_x, column(3 + k), column(8 + k)), both)
            z_in = jnp.where(off_z == k, wz, z_in)
            tails = jnp.where(off_t == k, wz, tails)
        wz_in[...] = z_in
        both = jnp.where(in_xy, both, 0.0)
        hi = both.astype(BF16).astype(F32)
        mid = (both - hi).astype(BF16).astype(F32)
        table = jnp.concatenate([(hi + pltpu.roll(mid, 64, 1)).astype(BF16), (both - hi - mid).astype(BF16)], axis=1)

        def weights_at(lo, n):
            return dot16(table, EX[:, lo:lo + n]) * dot16(table, EY[:, lo:lo + n])

        W[...], W_lo[...] = split(weights_at(0, inside))
        n = V.shape[1]
        hi, lo = split(weights_at(inside, W_ring))
        V[...], V_lo[...] = hi[:, 0:n], lo[:, 0:n]
        k = cy + 8
        hi, lo = split(dot16(table, EY[:, inside + W_ring:inside + W_ring + 128]))
        Wy[:, 0:k] = hi[:, 0:k]
        Wy[:, k:2 * k] = hi[:, 0:k]
        Wy[:, 2 * k:3 * k] = lo[:, 0:k]
        at_x = dot16(table, EX[:, inside + W_ring:])
        for g in range(wzx.shape[0]):
            wzx[g] = tails * at_x[:, g * 128:(g + 1) * 128]

    z_ways = sorted((way for way in DIRS if way[2]), key=lambda way: -sum(map(abs, way)))
    flat_ways = [way for way in DIRS if way[0] and way[1] and not way[2]] + YW

    def half(h, last):
        m, sp, s, d = parts(h)
        hi, lo = split(T[m, pl.ds(s, 2), 2:2 + cx, y0:y1, :].reshape(2 * cx * cy, cz))
        DZ[...] = dot16(jnp.concatenate([hi, lo], axis=1), inner[...]).reshape(2, cx, cy, cz)
        if not last:
            @pl.when(h == 1)
            def _():
                for k in range(2, min(3, nz)):
                    z_stage(k)

            @pl.when(h == 2)
            def _():
                for k in range(3, nz):
                    z_stage(k)
                y_stage(0)

            @pl.when(h == 3)
            def _():
                for k in range(1, min(2, ny)):
                    y_stage(k)

            @pl.when(h == 4)
            def _():
                for k in range(2, ny):
                    y_stage(k)
                for d in range(1, group):
                    request(d).start()

        recv_face(h, ZW)
        for g in range(cx // per):
            merged = jnp.where(tail < 2, zr[h, 0, g], zr[h, 1, g])
            l2, r2 = pltpu.roll(merged, cz - 2, 1), pltpu.roll(merged, 2, 1)
            l1, r1 = pltpu.roll(merged, cz - 1, 1), pltpu.roll(merged, 1, 1)
            fix = (jnp.where(tail < 2, -l2, r2)
                   + 8.0 * (jnp.where(tail == 1, l1, 0.0) - jnp.where(tail == 2, r1, 0.0)))
            for i in range(per):
                for q in range(2):
                    b = i * 8 + q * 4
                    DZ[q, g * per + i] = DZ[q, g * per + i] + jnp.where(
                        edge, pltpu.roll(fix, (2 * cz - b - 2) % cz, 1), 0.0)
        recv_face(h, YW)
        for q, c in enumerate((0, 2)):
            T[m, s + c, 2:2 + cx, y0 - 2:y0, :] = yr[h, 0, :, 2 * q:2 * q + 2, :]
            T[m, s + c, 2:2 + cx, y1:y1 + 2, :] = yr[h, 1, :, 2 * q:2 * q + 2, :]
        scale = step_size / jnp.asarray(m + 1, F32)
        plain = -scale / 12.0
        strips = [zfs[g] if h == 7 else jnp.zeros((cy, cz), F32) for g in range(cx // wide)] if last else []

        def plane(px):
            def d_x(c):
                at = lambda o: T[m, s + c, 2 + px + o, y0:y1, :]
                return (at(-2) - at(2)) + 8.0 * (at(1) - at(-1))

            def d_y(c):
                at = lambda o: T[m, s + c, 2 + px, y0 + o:y1 + o, :]
                return (at(-2) - at(2)) + 8.0 * (at(1) - at(-1))

            by = jnp.where(sp == 0, inv[px] * scale, plain)
            rates = [(d_y(2) - DZ[1, px]) * by, (DZ[0, px] - d_x(2)) * by, (d_x(1) - d_y(0)) * by]
            for c in range(3):
                total = F[d + c, px] + rates[c]
                F[d + c, px] = total
                if last:
                    rates[c] = total
                else:
                    T[m + 1, d + c, 2 + px, y0:y1, :] = rates[c]
            if last:
                g, i = px // wide, px % wide
                for c in range(3):
                    b = i * 32 + (d + c) * 4
                    strips[g] = jnp.where(lane // 4 == b // 4, pltpu.roll(rates[c], (b + 2) % cz, 1), strips[g])

        for px in range(2, cx - 2):
            plane(px)
        recv_face(h, XW)
        for px in (0, 1, cx - 2, cx - 1):
            plane(px)
        if last:
            j = h - 6
            for g, strip in enumerate(strips):
                zfs[g] = strip
                if j == 1:
                    zys[0, g] = strip[0:2]
                    zys[1, g] = strip[cy - 2:cy]
            if j == 1:
                start_final(j, z_ways)
            start_final(j, XW)
            for k, lo in ((0, 0), (1, cy - 2)):
                for c in range(3):
                    for px in range(cx):
                        yfs[j, k, c, px // 2, px % 2 * 2:px % 2 * 2 + 2, :] = F[d + c, px, lo:lo + 2, :]
            start_final(j, flat_ways)
        else:
            start_face(h + 2, XW)
            pack_y(h + 2)
            start_face(h + 2, YW)
            pack_z(h + 2)
            start_face(h + 2, ZW)

    def body(h, carry):
        half(h, False)
        return carry

    lax.fori_loop(0, 6, body, 0)
    half(6, True)
    half(7, True)

    build()
    depth = cx * cy

    def apply(w, w_lo, block):
        hi, lo = split(block)
        return dot16(w[...], hi) + dot16(w[...], lo) + dot16(w_lo[...], hi)

    for c in (3, 4, 5, 0, 1, 2):
        part[c] = apply(W, W_lo, F[c].reshape(depth, cz))

    slot_row = lax.broadcasted_iota(jnp.int32, (slots, cz), 0)
    slot_lane = lax.broadcasted_iota(jnp.int32, (slots, cz), 1)
    target = slot_row // served_rows * per_owner + slot_row % per_owner - slot_lane
    result = jnp.zeros((slots, cz), F32)
    ktail = lax.broadcasted_iota(jnp.int32, (1, cz), 1) % 4 < 2
    for j in range(2):
        d = 3 * (1 - j)
        for way in flat_ways + XW:
            @pl.when(has[negate(way)])
            def _():
                final_copy(j, way).wait_recv()

        blocks = []
        for c in range(3):
            pieces = ([XR[d + c].reshape(4 * cy, cz)]
                      + [YR[d + c, k, i] for k in range(2) for i in range(cx // 2)]
                      + [XYR[d + c, kx, ky] for kx in range(2) for ky in range(2)])
            blocks.append(jnp.concatenate(pieces, axis=0))
        added = apply(V, V_lo, jnp.concatenate(blocks, axis=1))
        for c in range(3):
            both = (part[d + c] + added[:, c * cz:(c + 1) * cz]) * wz_in[...]
            result = jnp.where(target == -(d + c) * cap, jnp.sum(both, axis=1, keepdims=True), result)

    for way in z_ways:
        @pl.when(has[negate(way)])
        def _():
            final_copy(1, way).wait_recv()

    def ring(centre, low, high):
        return jnp.concatenate(
            [jnp.where(ktail, a[0], a[1]) for a in (centre, low, high)] + [jnp.zeros((4, cz), F32)], axis=0)

    strips = [ring([ZX[0, k] for k in range(2)], [ZXY[0, 0, k] for k in range(2)],
                   [ZXY[0, 1, k] for k in range(2)])]
    for g in range(cx // wide):
        strips.append(ring([ZR[k, g] for k in range(2)], [ZY[0, k, g] for k in range(2)],
                           [ZY[1, k, g] for k in range(2)]))
    strips.append(ring([ZX[1, k] for k in range(2)], [ZXY[1, 0, k] for k in range(2)],
                       [ZXY[1, 1, k] for k in range(2)]))
    hi, lo = split(jnp.concatenate(strips, axis=1))
    zsum = dot16(Wy[...], jnp.concatenate([hi, lo, hi], axis=0))
    zpart = jnp.zeros((slots, cz), F32)
    for g in range(len(strips)):
        zpart = zpart + zsum[:, g * cz:(g + 1) * cz] * wzx[g]
    zsum = dot16(jnp.concatenate(split(zpart), axis=1), gather[...])
    result = result + jnp.where((target + slot_lane) == slot_lane % cap, zsum, 0.0)

    folded = result[0:served_rows]
    for b in range(1, BLOCKS):
        folded = folded + result[b * served_rows:(b + 1) * served_rows]
    for o in range(group):
        ans[o] = jnp.sum(folded[o * per_owner:(o + 1) * per_owner], axis=0, keepdims=True)
    for d in range(1, group):
        answer(d).start()
    ansr[me] = ans[me]

    def drain(h, carry):
        for way in FACES:
            @pl.when(has[way])
            def _():
                face_copy(h, way).wait_send()
        return carry

    lax.fori_loop(0, 8, drain, 0)
    for j in range(2):
        for way in DIRS:
            if j == 1 or not way[2]:
                @pl.when(has[way])
                def _():
                    final_copy(j, way).wait_send()
    for d in range(1, group):
        request(d).wait_send()
    for d in range(1, group):
        answer(d).wait_recv()
    for d in range(1, group):
        answer(d).wait_send()


def finish_kernel(cap, F, ansr, hits_t, slot_t, out, recept, values, sem):
    store = pltpu.make_async_copy(F, out, sem.at[0])
    store.start()
    group = ansr.shape[0]
    got = jnp.concatenate([ansr[o] for o in range(group)], axis=0)
    hi, low = split(got)
    mid, lo = split(got - hi.astype(F32))
    hits = hits_t[...].astype(BF16)
    picked = lax.dot_general(jnp.concatenate([hi, mid, lo], axis=0), jnp.concatenate([hits] * 3, axis=0),
                             (((0,), (0,)), ((), ())), preferred_element_type=F32)
    at = lax.broadcasted_iota(jnp.int32, picked.shape, 0) % cap
    picked = jnp.where(at == slot_t[...].astype(jnp.int32), picked, 0.0)
    for c in range(6):
        values[c:c + 1] = jnp.sum(picked[c * cap:(c + 1) * cap], axis=0, keepdims=True)
    small = pltpu.make_async_copy(values, recept, sem.at[1])
    small.start()
    store.wait()
    small.wait()


def local(sizes, fields, permittivity, donor_owner, donor_base, donor_weights):
    nx, ny, nz = sizes
    cx, cy, cz = permittivity.shape
    rows = donor_owner.shape[0]
    group = ny * nz
    cap = 2 * rows // group
    slots = group * cap
    per_owner = cap // BLOCKS
    vmem = pltpu.VMEM
    dma = pltpu.SemaphoreType.DMA
    yrows = cy + 16
    strips = cx * 8 // cz
    wide = cx * 32 // cz
    outer = 4 * cy + 4 * cx + 16
    ring = -(-outer // 128) * 128
    new, *answers = pl.pallas_call(
        functools.partial(kernel, (nx, ny, nz, cap), ring),
        out_shape=(
            vmem(fields.shape, F32),
            vmem((group, 1, 128), F32),
            vmem((group, rows), F32),
            vmem((1, rows), F32),
        ),
        in_specs=[pl.BlockSpec(memory_space=pl.ANY)] * 5,
        out_specs=(pl.BlockSpec(memory_space=vmem),) * 4,
        scratch_shapes=[
            vmem((1, rows), jnp.int32),
            vmem((3, rows), jnp.int32),
            vmem((15, rows), F32),
            vmem((5, 6, cx + 4, yrows, cz), F32),
            vmem((cx, cy, cz), F32),
            vmem((8, 2, cx, 4, cz), F32),
            vmem((8, 2, cx, 4, cz), F32),
            vmem((8, strips, cy, cz), F32),
            vmem((8, 2, strips, cy, cz), F32),
            vmem((2, cx, cy, cz), F32),
            vmem((2, 2, 3, cx // 2, 4, cz), F32),
            vmem((wide, cy, cz), F32),
            vmem((2, wide, 2, cz), F32),
            vmem((6, 2, 2, cy, cz), F32),
            vmem((6, 2, cx // 2, 4, cz), F32),
            vmem((6, 2, 2, 4, cz), F32),
            vmem((2, wide, cy, cz), F32),
            vmem((2, 2, cy, cz), F32),
            vmem((2, 2, wide, 2, cz), F32),
            vmem((2, 2, 2, 2, cz), F32),
            vmem((128, rows), F32),
            vmem((2 * cz, cz), BF16),
            vmem((2 * cz, cz), BF16),
            vmem((256, cx * cy + ring + 128 * (wide + 2)), BF16),
            vmem((256, cx * cy + ring + 128), BF16),
            vmem((group, per_owner, 128), F32),
            vmem((group, per_owner, 128), F32),
            vmem((group, 1, 128), F32),
            vmem((slots, cx * cy), BF16),
            vmem((slots, cx * cy), BF16),
            vmem((slots, outer), BF16),
            vmem((slots, outer), BF16),
            vmem((slots, 3 * (cy + 8)), BF16),
            vmem((wide + 2, slots, cz), F32),
            vmem((slots, cz), F32),
            vmem((6, slots, cz), F32),
            pltpu.SemaphoreType.REGULAR((2,)),
            pltpu.SemaphoreType.REGULAR((2,)),
            dma((8,)),
            dma((8, 6)),
            dma((8, 6)),
            dma((2, 26)),
            dma((2, 26)),
            dma((group,)),
            dma((group,)),
            dma((group,)),
            dma((group,)),
        ],
        compiler_params=pltpu.CompilerParams(
            collective_id=0, has_side_effects=True, vmem_limit_bytes=60 * 1024 * 1024
        ),
    )(fields, permittivity, donor_owner.T, donor_base.T, donor_weights.T)
    return pl.pallas_call(
        functools.partial(finish_kernel, cap),
        out_shape=(
            jax.ShapeDtypeStruct(fields.shape, F32),
            jax.ShapeDtypeStruct((6, rows), F32),
        ),
        in_specs=[pl.BlockSpec(memory_space=vmem)] * 4,
        out_specs=(pl.BlockSpec(memory_space=pl.ANY),) * 2,
        scratch_shapes=[vmem((6, rows), F32), dma((2,))],
        compiler_params=pltpu.CompilerParams(vmem_limit_bytes=2 * 1024 * 1024),
    )(new, *answers)


def solution(mesh):
    sizes = (mesh.shape["gx"], mesh.shape["gy"], mesh.shape["gz"])
    placed = (
        P(None, "gx", "gy", "gz"),
        P("gx", "gy", "gz"),
        P(("gx", "gy", "gz"), None),
        P(("gx", "gy", "gz"), None),
        P(("gx", "gy", "gz"), None),
    )
    return jax.shard_map(
        functools.partial(local, sizes),
        mesh=mesh,
        in_specs=placed,
        out_specs=(P(None, "gx", "gy", "gz"), P(None, ("gx", "gy", "gz"))),
        check_vma=False,
    )
```

```python
import functools

import jax
import jax.numpy as jnp
from jax import lax
from jax.experimental import pallas as pl
from jax.experimental.pallas import tpu as pltpu
from jax.sharding import PartitionSpec as P

step_size = 0.25
MESH = pl.DeviceIdType.MESH
F32 = jnp.float32
BF16 = jnp.bfloat16
HI = lax.Precision.HIGHEST
BLOCKS = 4
FEATURES = 32
DIRS = [(a, b, c) for a in (-1, 0, 1) for b in (-1, 0, 1) for c in (-1, 0, 1) if (a, b, c) != (0, 0, 0)]
FACES = [(-1, 0, 0), (1, 0, 0), (0, -1, 0), (0, 1, 0), (0, 0, -1), (0, 0, 1)]


def dot(a, b, dims=((1,), (0,))):
    return lax.dot_general(a, b, (dims, ((), ())), precision=HI, preferred_element_type=F32)


def split(a):
    hi = a.astype(BF16)
    return hi, (a - hi.astype(F32)).astype(BF16)


def dot16(a, b):
    return lax.dot_general(a, b, (((1,), (0,)), ((), ())), preferred_element_type=F32)


def negate(way):
    return tuple(-a for a in way)


def slot_of(a):
    return 0 if a < 0 else 1


def kernel(
    sizes, W_ring, fields, eps, owner_in, bases_in, weights_in, F, ansr, hits_t, slot_t,
    owner, bases, weights, T, inv, ys, yr, zs, zr, DZ, R,
    yfs, zfs, zys, XR, YR, XYR, ZR, ZX, ZY, ZXY,
    data_t, inner, gather, EX, EY, req, reqr, ans, W, V, Wy, wzx, wz_in, part, saved,
    z_sem, y_sem, load_sem, send, recv, fsend, frecv, rsend, rrecv, asend, arecv,
):
    nx, ny, nz, cap = sizes
    group = ny * nz
    per_owner = cap // BLOCKS
    cx, cy, cz = eps.shape
    rows = owner.shape[1]
    slots = group * cap
    x, y, z = lax.axis_index("gx"), lax.axis_index("gy"), lax.axis_index("gz")
    me = y * nz + z
    y0, y1 = 8, 8 + cy

    loads = [
        pltpu.make_async_copy(fields.at[pl.ds(3, 3)], T.at[0, pl.ds(3, 3), pl.ds(2, cx), pl.ds(8, cy), :], load_sem.at[0]),
        pltpu.make_async_copy(owner_in, owner, load_sem.at[1]),
        pltpu.make_async_copy(bases_in, bases, load_sem.at[2]),
        pltpu.make_async_copy(weights_in, weights, load_sem.at[3]),
        pltpu.make_async_copy(eps, inv, load_sem.at[4]),
        pltpu.make_async_copy(fields, F, load_sem.at[5]),
        pltpu.make_async_copy(fields.at[pl.ds(0, 3)], T.at[0, pl.ds(0, 3), pl.ds(2, cx), pl.ds(8, cy), :], load_sem.at[6]),
    ]
    for copy in (loads[0], loads[6], *loads[1:5]):
        copy.start()

    has = {
        (-1, 0, 0): x > 0, (1, 0, 0): x < nx - 1, (0, -1, 0): y > 0,
        (0, 1, 0): y < ny - 1, (0, 0, -1): z > 0, (0, 0, 1): z < nz - 1,
    }
    for way in DIRS:
        found = None
        for axis in range(3):
            if way[axis]:
                face = tuple(way[a] if a == axis else 0 for a in range(3))
                found = has[face] if found is None else found & has[face]
        has[way] = found

    def dev(way):
        return (x + way[0], y + way[1], z + way[2])

    barrier = pltpu.get_barrier_semaphore()
    others = []
    for d in range(1, group):
        t = lax.rem(me + d, group)
        others.append((x, t // nz, lax.rem(t, nz)))
    expected = jnp.int32(0)
    for way in FACES:
        expected = expected + has[way].astype(jnp.int32)

        @pl.when(has[way])
        def _():
            pl.semaphore_signal(barrier, inc=1, device_id=dev(way), device_id_type=MESH)

    def line_stage(k, at, count, sems, up):
        down = negate(up)
        for here, side, way in ((at == k, 0, up), (at == count - 1 - k, 1, down)):
            @pl.when(here)
            def _():
                if k > 0:
                    pl.semaphore_wait(sems.at[side], 1)
                if k < count - 1:
                    pl.semaphore_signal(sems.at[side], inc=1, device_id=dev(way), device_id_type=MESH)

    def z_stage(k):
        line_stage(k, z, nz, z_sem, (0, 0, 1))

    def y_stage(k):
        line_stage(k, y, ny, y_sem, (0, 1, 0))

    lane = lax.broadcasted_iota(jnp.int32, (cy, cz), 1)
    lane1 = lax.broadcasted_iota(jnp.int32, (1, cz), 1)

    def remote(src, dst, s, r, target):
        return pltpu.make_async_remote_copy(
            src_ref=src, dst_ref=dst, send_sem=s, recv_sem=r, device_id=target, device_id_type=MESH)

    def request(d):
        return remote(req.at[(me + d) % group], reqr.at[me], rsend.at[d], rrecv.at[d], others[d - 1])

    def answer(d):
        return remote(ans.at[(me + d) % group], ansr.at[me], asend.at[d], arecv.at[d], others[d - 1])

    def parts(h):
        m = h // 2
        sp = (m + h % 2) % 2
        return m, sp, 3 * (1 - sp), 3 * sp

    def face_copy(h, way):
        m, sp, s, d = parts(h)
        i = FACES.index(way)
        if way[0]:
            lo_src, lo_dst = (2, cx + 2) if way[0] < 0 else (cx, 0)
            src = T.at[m, pl.ds(s + 1, 2), pl.ds(lo_src, 2), pl.ds(8, cy)]
            dst = T.at[m, pl.ds(s + 1, 2), pl.ds(lo_dst, 2), pl.ds(8, cy)]
        elif way[1]:
            k = slot_of(way[1])
            src, dst = ys.at[h, k], yr.at[h, 1 - k]
        else:
            src, dst = zs.at[h], zr.at[h, 1 - slot_of(way[2])]
        return remote(src, dst, send.at[h, i], recv.at[h, i], dev(way))

    def start_face(h, ways, also=None):
        for way in ways:
            @pl.when(has[way] if also is None else has[way] & also)
            def _():
                face_copy(h, way).start()

    def recv_face(h, ways):
        for way in ways:
            @pl.when(has[negate(way)])
            def _():
                face_copy(h, way).wait_recv()

    XW, YW, ZW = FACES[0:2], FACES[2:4], FACES[4:6]
    per = cz // 8

    def pack_y(h):
        m, sp, s, d = parts(h)
        for q, c in enumerate((0, 2)):
            ys[h, 0, :, 2 * q:2 * q + 2, :] = T[m, s + c, 2:2 + cx, y0:y0 + 2, :]
            ys[h, 1, :, 2 * q:2 * q + 2, :] = T[m, s + c, 2:2 + cx, y1 - 2:y1, :]

    def pack_z(h):
        m, sp, s, d = parts(h)
        for g in range(cx // per):
            strip = jnp.zeros((cy, cz), F32)
            for i in range(per):
                for q in range(2):
                    b = i * 8 + q * 4
                    strip = jnp.where(lane // 4 == b // 4,
                                      pltpu.roll(T[m, s + q, 2 + g * per + i, y0:y1, :], (b + 2) % cz, 1), strip)
            zs[h, g] = strip

    loads[0].wait()
    pack_y(0)
    pl.semaphore_wait(barrier, expected)
    for h in range(2):
        if h == 1:
            loads[6].wait()
            loads[5].start()
            pack_y(h)
        start_face(h, XW, y % 2 == 0)
        start_face(h, YW)
        pack_z(h)
        start_face(h, ZW)
        start_face(h, XW, y % 2 == 1)
    z_stage(0)

    def clear(ref):
        ref[...] = jnp.zeros(ref.shape, F32)

    for way in DIRS:
        kx, ky, kz = (slot_of(a) for a in way)
        here = tuple(abs(a) for a in way)

        @pl.when(jnp.logical_not(has[way]))
        def _():
            if here == (1, 0, 0):
                for m in range(4):
                    clear(T.at[m, :, pl.ds(kx * (cx + 2), 2), pl.ds(8, cy)])
                clear(XR.at[:, kx])
            elif here == (0, 1, 0):
                clear(yr.at[:, ky])
                clear(YR.at[:, ky])
            elif here == (0, 0, 1):
                clear(zr.at[:, kz])
                clear(ZR.at[kz])
            elif here == (1, 1, 0):
                clear(XYR.at[:, kx, ky])
            elif here == (1, 0, 1):
                clear(ZX.at[kx, kz])
            elif here == (0, 1, 1):
                clear(ZY.at[ky, kz])
            else:
                clear(ZXY.at[kx, ky, kz])

    zi = lax.broadcasted_iota(jnp.int32, (2 * cz, cz), 0) % cz
    zo = lax.broadcasted_iota(jnp.int32, (2 * cz, cz), 1)
    delta = zi - zo
    inner[...] = (jnp.where(delta == -2, 1.0, 0.0) - jnp.where(delta == 2, 1.0, 0.0)
                  + jnp.where(delta == 1, 8.0, 0.0) - jnp.where(delta == -1, 8.0, 0.0)).astype(BF16)

    for copy in loads[1:4]:
        copy.wait()
    for b in range(BLOCKS):
        at = b * FEATURES
        data_t[at:at + 3] = bases[...].astype(F32)
        data_t[at + 3:at + 18] = weights[...]
        data_t[at + 18:at + FEATURES] = jnp.zeros((FEATURES - 18, rows), F32)
    own = owner[...]
    hits = jnp.where(lax.broadcasted_iota(jnp.int32, (group, rows), 0) == own, 1.0, 0.0)
    hits_t[...] = hits
    earlier = dot16(hits.astype(BF16), (lax.broadcasted_iota(jnp.int32, (rows, rows), 0)
                                        < lax.broadcasted_iota(jnp.int32, (rows, rows), 1)).astype(BF16))
    slot_f = jnp.sum(earlier * hits, axis=0, keepdims=True)
    slot_t[...] = slot_f
    slot = slot_f.astype(jnp.int32)
    block = lax.broadcasted_iota(jnp.int32, (BLOCKS * FEATURES, rows), 0) // FEATURES
    placed = jnp.where(block == slot // per_owner, data_t[...], 0.0)
    flat = own * per_owner + slot % per_owner
    perm = (flat == lax.broadcasted_iota(jnp.int32, (group * per_owner, rows), 0)).astype(F32)
    packed = dot(perm, placed, ((1,), (1,)))
    for o in range(group):
        req[o] = packed[o * per_owner:(o + 1) * per_owner]
    reqr[me] = req[me]
    loads[4].wait()
    inv[...] = 1.0 / (12.0 * inv[...])
    loads[5].wait()
    here_x = lax.broadcasted_iota(jnp.int32, (64, 128), 0)
    inside = cx * cy
    ring_x, ring_y = 4 * cy, 4 * cx

    def one_hot(ref, lo, hot):
        hot = jnp.where(hot, 1.0, 0.0).astype(BF16)
        for k in range(3):
            ref[k * 64:(k + 1) * 64, lo:lo + 128] = hot
        ref[192:256, lo:lo + 128] = jnp.zeros((64, 128), BF16)

    def place(lo, xe, ye):
        one_hot(EX, lo, here_x == xe)
        one_hot(EY, lo, here_x - 32 == ye)

    for lo in range(0, inside, 128):
        li = lo + lane1
        place(lo, li // cy + 2, li % cy + 2)
    for lo in range(0, W_ring, 128):
        li = lo + lane1
        i1 = li % (2 * cy)
        l2 = li - ring_x
        l3 = li - ring_x - ring_y
        xe = jnp.where(
            l2 < 0, i1 // cy + jnp.where(li >= 2 * cy, cx + 2, 0),
            jnp.where(l3 < 0, (l2 % (2 * cx)) // 2 + 2, (l3 % 4) // 2 + jnp.where(l3 >= 8, cx + 2, 0)))
        ye = jnp.where(
            l2 < 0, i1 % cy + 2,
            jnp.where(l3 < 0, l2 % 2 + jnp.where(l2 >= 2 * cx, cy + 2, 0),
                      l3 % 2 + jnp.where(l3 % 8 >= 4, cy + 2, 0)))
        place(inside + lo, jnp.where(l3 < 16, xe, -100), jnp.where(l3 < 16, ye, -100))
    ye = jnp.where(lane1 < cy, lane1 + 2, jnp.where(lane1 < cy + 2, lane1 - cy, lane1))
    one_hot(EY, inside + W_ring, here_x - 32 == jnp.where(lane1 < cy + 4, ye, -100))
    wide = cz // 32
    for g in range(wzx.shape[0]):
        xe = lane1 // 32 + 2 + wide * (g - 1)
        one_hot(EX, inside + W_ring + 128 * g, here_x == jnp.where(xe < 32, xe, -100))
    comp_row = lax.broadcasted_iota(jnp.int32, (2 * cz, cz), 0) % 32 // 4
    comp_col = lax.broadcasted_iota(jnp.int32, (2 * cz, cz), 1) // cap
    gather[...] = jnp.where((comp_row == comp_col) & (comp_row < 6), 1.0, 0.0).astype(BF16)
    for k in range(1, min(2, nz)):
        z_stage(k)

    edge = (lane < 2) | (lane >= cz - 2)
    tail = lane % 4

    def final_copy(j, way):
        i = DIRS.index(way)
        d = 3 * (1 - j)
        here = tuple(abs(a) for a in way)
        kx, ky, kz = (slot_of(a) for a in way)
        nx_, ny_, nz_ = 1 - kx, 1 - ky, 1 - kz
        strip = kx * (zfs.shape[0] - 1)
        if here == (1, 0, 0):
            src, dst = F.at[pl.ds(d, 3), pl.ds(kx * (cx - 2), 2)], XR.at[pl.ds(d, 3), nx_]
        elif here == (0, 1, 0):
            src, dst = yfs.at[j, ky], YR.at[pl.ds(d, 3), ny_]
        elif here == (0, 0, 1):
            src, dst = zfs, ZR.at[nz_]
        elif here == (1, 1, 0):
            src = yfs.at[j, ky, :, kx * (cx // 2 - 1)]
            dst = XYR.at[pl.ds(d, 3), nx_, ny_]
        elif here == (1, 0, 1):
            src, dst = zfs.at[strip], ZX.at[nx_, nz_]
        elif here == (0, 1, 1):
            src, dst = zys.at[ky], ZY.at[ny_, nz_]
        else:
            src, dst = zys.at[ky, strip], ZXY.at[nx_, ny_, nz_]
        return remote(src, dst, fsend.at[j, i], frecv.at[j, i], dev(way))

    def start_final(j, ways, also=None):
        for way in ways:
            @pl.when(has[way] if also is None else has[way] & also)
            def _():
                final_copy(j, way).start()

    served_rows = group * per_owner

    def served_table():
        if per_owner % 8 == 0:
            table = reqr[...].reshape(served_rows, 128)
        else:
            table = jnp.concatenate([reqr[o] for o in range(group)], axis=0)
        turned = [table] + [pltpu.roll(table, 128 - b * FEATURES, 1) for b in range(1, BLOCKS)]
        return jnp.concatenate(turned, axis=0)

    def build():
        for d in range(1, group):
            request(d).wait_recv()
        served = served_table()

        def column(k):
            return jnp.broadcast_to(served[:, k:k + 1], (slots, 128))

        li = lax.broadcasted_iota(jnp.int32, (slots, 128), 1)
        flat_lane = li.astype(F32)
        bx, by, bz = column(0), column(1), column(2)
        in_x, in_xy = li < 32, li < 64
        off = jnp.where(in_x, flat_lane - bx, flat_lane - 32.0 - by)
        t = li % 4
        off_z = flat_lane + 2.0 - bz
        off_t = jnp.where(t < 2, t, cz + t).astype(F32) - bz
        both = jnp.zeros((slots, 128), F32)
        z_in = jnp.zeros((slots, 128), F32)
        tails = jnp.zeros((slots, 128), F32)
        for k in range(5):
            wz = column(13 + k)
            both = jnp.where(off == k, jnp.where(in_x, column(3 + k), column(8 + k)), both)
            z_in = jnp.where(off_z == k, wz, z_in)
            tails = jnp.where(off_t == k, wz, tails)
        wz_in[...] = z_in
        both = jnp.where(in_xy, both, 0.0)
        hi = both.astype(BF16).astype(F32)
        mid = (both - hi).astype(BF16).astype(F32)
        table = jnp.concatenate([(hi + pltpu.roll(mid, 64, 1)).astype(BF16), (both - hi - mid).astype(BF16)], axis=1)

        def weights_at(lo, n):
            return dot16(table, EX[:, lo:lo + n]) * dot16(table, EY[:, lo:lo + n])

        hi, lo = split(weights_at(0, inside))
        for k, piece in enumerate((hi, hi, lo)):
            W[:, k * inside:(k + 1) * inside] = piece
        n = V.shape[1] // 3
        hi, lo = split(weights_at(inside, W_ring))
        for k, piece in enumerate((hi, hi, lo)):
            V[:, k * n:(k + 1) * n] = piece[:, 0:n]
        k = cy + 8
        hi, lo = split(dot16(table, EY[:, inside + W_ring:inside + W_ring + 128]))
        Wy[:, 0:k] = hi[:, 0:k]
        Wy[:, k:2 * k] = hi[:, 0:k]
        Wy[:, 2 * k:3 * k] = lo[:, 0:k]
        at_x = dot16(table, EX[:, inside + W_ring:])
        for g in range(wzx.shape[0]):
            wzx[g] = tails * at_x[:, g * 128:(g + 1) * 128]

    z_ways = sorted((way for way in DIRS if way[2]), key=lambda way: -sum(map(abs, way)))
    flat_ways = [way for way in DIRS if way[0] and way[1] and not way[2]] + YW

    def half(h, last):
        m, sp, s, d = parts(h)
        hi, lo = split(T[m, pl.ds(s, 2), 2:2 + cx, y0:y1, :].reshape(2 * cx * cy, cz))
        DZ[...] = dot16(jnp.concatenate([hi, lo], axis=1), inner[...]).reshape(2, cx, cy, cz)
        if not last:
            @pl.when(h == 1)
            def _():
                for k in range(2, min(3, nz)):
                    z_stage(k)

            @pl.when(h == 2)
            def _():
                for k in range(3, nz):
                    z_stage(k)
                y_stage(0)

            @pl.when(h == 3)
            def _():
                for k in range(1, min(2, ny)):
                    y_stage(k)

            @pl.when(h == 4)
            def _():
                for k in range(2, ny):
                    y_stage(k)
                for d in range(1, group):
                    request(d).start()

        recv_face(h, YW)
        for q, c in enumerate((0, 2)):
            T[m, s + c, 2:2 + cx, y0 - 2:y0, :] = yr[h, 0, :, 2 * q:2 * q + 2, :]
            T[m, s + c, 2:2 + cx, y1:y1 + 2, :] = yr[h, 1, :, 2 * q:2 * q + 2, :]
        scale = step_size / jnp.asarray(m + 1, F32)
        plain = -scale / 12.0
        strips = [zfs[g] if h == 7 else jnp.zeros((cy, cz), F32) for g in range(cx // wide)] if last else []

        def by_of(px):
            return jnp.where(sp == 0, inv[px] * scale, plain)

        def rates_of(px):
            def d_x(c):
                at = lambda o: T[m, s + c, 2 + px + o, y0:y1, :]
                return (at(-2) - at(2)) + 8.0 * (at(1) - at(-1))

            def d_y(c):
                at = lambda o: T[m, s + c, 2 + px, y0 + o:y1 + o, :]
                return (at(-2) - at(2)) + 8.0 * (at(1) - at(-1))

            return [d_y(2) - DZ[1, px], DZ[0, px] - d_x(2), d_x(1) - d_y(0)]

        def finish_plane(px, rates, by, comps=range(3)):
            for c in comps:
                rate = rates[c] * by
                total = F[d + c, px] + rate
                F[d + c, px] = total
                if last:
                    g, i = px // wide, px % wide
                    b = i * 32 + (d + c) * 4
                    strips[g] = jnp.where(lane // 4 == b // 4, pltpu.roll(total, (b + 2) % cz, 1), strips[g])
                else:
                    T[m + 1, d + c, 2 + px, y0:y1, :] = rate

        for px in range(2, cx - 2):
            rates = rates_of(px)
            for c in range(2):
                R[c, px] = rates[c]
            finish_plane(px, rates, by_of(px), (2,))
        recv_face(h, ZW)
        for g in range(cx // per):
            merged = jnp.where(tail < 2, zr[h, 0, g], zr[h, 1, g])
            l2, r2 = pltpu.roll(merged, cz - 2, 1), pltpu.roll(merged, 2, 1)
            l1, r1 = pltpu.roll(merged, cz - 1, 1), pltpu.roll(merged, 1, 1)
            fix = (jnp.where(tail < 2, -l2, r2)
                   + 8.0 * (jnp.where(tail == 1, l1, 0.0) - jnp.where(tail == 2, r1, 0.0)))

            def at_edge(px, q):
                b = px % per * 8 + q * 4
                return jnp.where(edge, pltpu.roll(fix, (2 * cz - b - 2) % cz, 1), 0.0)

            for px in range(g * per, (g + 1) * per):
                if px in (0, 1, cx - 2, cx - 1):
                    for q in range(2):
                        DZ[q, px] = DZ[q, px] + at_edge(px, q)
                else:
                    finish_plane(px, [R[0, px] - at_edge(px, 1), R[1, px] + at_edge(px, 0)], by_of(px), (0, 1))
        recv_face(h, XW)
        for px in (0, 1, cx - 2, cx - 1):
            finish_plane(px, rates_of(px), by_of(px))
        if last:
            j = h - 6
            for g, strip in enumerate(strips):
                zfs[g] = strip
                if j == 1:
                    zys[0, g] = strip[0:2]
                    zys[1, g] = strip[cy - 2:cy]
            if j == 1:
                start_final(j, z_ways)
            start_final(j, XW, y % 2 == 0)
            for k, lo in ((0, 0), (1, cy - 2)):
                for c in range(3):
                    for px in range(cx):
                        yfs[j, k, c, px // 2, px % 2 * 2:px % 2 * 2 + 2, :] = F[d + c, px, lo:lo + 2, :]
            start_final(j, flat_ways)
            start_final(j, XW, y % 2 == 1)
        else:
            start_face(h + 2, XW, y % 2 == 0)
            pack_y(h + 2)
            start_face(h + 2, YW)
            pack_z(h + 2)
            start_face(h + 2, ZW)
            start_face(h + 2, XW, y % 2 == 1)

    def body(h, carry):
        half(h, False)
        return carry

    lax.fori_loop(0, 6, body, 0)
    half(6, True)
    half(7, True)

    build()
    depth = cx * cy

    def apply(w, block):
        hi, lo = split(block)
        return dot16(w[...], jnp.concatenate([hi, lo, hi], axis=0))

    for d in (3, 0):
        both = apply(W, jnp.concatenate([F[d + c].reshape(depth, cz) for c in range(3)], axis=1))
        for c in range(3):
            part[d + c] = both[:, c * cz:(c + 1) * cz]

    slot_row = lax.broadcasted_iota(jnp.int32, (slots, cz), 0)
    slot_lane = lax.broadcasted_iota(jnp.int32, (slots, cz), 1)
    target = slot_row // served_rows * per_owner + slot_row % per_owner - slot_lane
    result = jnp.zeros((slots, cz), F32)
    ktail = lax.broadcasted_iota(jnp.int32, (1, cz), 1) % 4 < 2
    def faces(j, result):
        d = 3 * (1 - j)
        blocks = []
        for c in range(3):
            pieces = ([XR[d + c].reshape(4 * cy, cz)]
                      + [YR[d + c, k, i] for k in range(2) for i in range(cx // 2)]
                      + [XYR[d + c, kx, ky] for kx in range(2) for ky in range(2)])
            blocks.append(jnp.concatenate(pieces, axis=0))
        added = apply(V, jnp.concatenate(blocks, axis=1))
        for c in range(3):
            both = (part[d + c] + added[:, c * cz:(c + 1) * cz]) * wz_in[...]
            result = jnp.where(target == -(d + c) * cap, jnp.sum(both, axis=1, keepdims=True), result)
        return result

    def recv_final(j, ways):
        for way in ways:
            @pl.when(has[negate(way)])
            def _():
                final_copy(j, way).wait_recv()

    def ring(centre, low, high):
        return jnp.concatenate(
            [jnp.where(ktail, a[0], a[1]) for a in (centre, low, high)] + [jnp.zeros((4, cz), F32)], axis=0)

    recv_final(0, flat_ways + XW)
    saved[...] = faces(0, result)
    recv_final(1, flat_ways + XW + z_ways)
    strips = [ring([ZX[0, k] for k in range(2)], [ZXY[0, 0, k] for k in range(2)],
                   [ZXY[0, 1, k] for k in range(2)])]
    for g in range(cx // wide):
        strips.append(ring([ZR[k, g] for k in range(2)], [ZY[0, k, g] for k in range(2)],
                           [ZY[1, k, g] for k in range(2)]))
    strips.append(ring([ZX[1, k] for k in range(2)], [ZXY[1, 0, k] for k in range(2)],
                       [ZXY[1, 1, k] for k in range(2)]))
    hi, lo = split(jnp.concatenate(strips, axis=1))
    zsum = dot16(Wy[...], jnp.concatenate([hi, lo, hi], axis=0))
    zpart = jnp.zeros((slots, cz), F32)
    for g in range(len(strips)):
        zpart = zpart + zsum[:, g * cz:(g + 1) * cz] * wzx[g]
    zsum = dot16(jnp.concatenate(split(zpart), axis=1), gather[...])
    result = faces(1, saved[...])
    result = result + jnp.where((target + slot_lane) == slot_lane % cap, zsum, 0.0)

    folded = result[0:served_rows]
    for b in range(1, BLOCKS):
        folded = folded + result[b * served_rows:(b + 1) * served_rows]
    for o in range(group):
        ans[o] = jnp.sum(folded[o * per_owner:(o + 1) * per_owner], axis=0, keepdims=True)
    for d in range(1, group):
        answer(d).start()
    ansr[me] = ans[me]

    def drain(h, carry):
        for way in FACES:
            @pl.when(has[way])
            def _():
                face_copy(h, way).wait_send()
        return carry

    lax.fori_loop(0, 8, drain, 0)
    for j in range(2):
        for way in DIRS:
            if j == 1 or not way[2]:
                @pl.when(has[way])
                def _():
                    final_copy(j, way).wait_send()
    for d in range(1, group):
        request(d).wait_send()
    for d in range(1, group):
        answer(d).wait_recv()
    for d in range(1, group):
        answer(d).wait_send()


def finish_kernel(cap, F, ansr, hits_t, slot_t, out, recept, values, sem):
    store = pltpu.make_async_copy(F, out, sem.at[0])
    store.start()
    group = ansr.shape[0]
    got = jnp.concatenate([ansr[o] for o in range(group)], axis=0)
    hi, low = split(got)
    mid, lo = split(got - hi.astype(F32))
    hits = hits_t[...].astype(BF16)
    picked = lax.dot_general(jnp.concatenate([hi, mid, lo], axis=0), jnp.concatenate([hits] * 3, axis=0),
                             (((0,), (0,)), ((), ())), preferred_element_type=F32)
    at = lax.broadcasted_iota(jnp.int32, picked.shape, 0) % cap
    picked = jnp.where(at == slot_t[...].astype(jnp.int32), picked, 0.0)
    for c in range(6):
        values[c:c + 1] = jnp.sum(picked[c * cap:(c + 1) * cap], axis=0, keepdims=True)
    small = pltpu.make_async_copy(values, recept, sem.at[1])
    small.start()
    store.wait()
    small.wait()


def local(sizes, fields, permittivity, donor_owner, donor_base, donor_weights):
    nx, ny, nz = sizes
    cx, cy, cz = permittivity.shape
    rows = donor_owner.shape[0]
    group = ny * nz
    cap = 2 * rows // group
    slots = group * cap
    per_owner = cap // BLOCKS
    vmem = pltpu.VMEM
    dma = pltpu.SemaphoreType.DMA
    yrows = cy + 16
    strips = cx * 8 // cz
    wide = cx * 32 // cz
    outer = 4 * cy + 4 * cx + 16
    ring = -(-outer // 128) * 128
    new, *answers = pl.pallas_call(
        functools.partial(kernel, (nx, ny, nz, cap), ring),
        out_shape=(
            vmem(fields.shape, F32),
            vmem((group, 1, 128), F32),
            vmem((group, rows), F32),
            vmem((1, rows), F32),
        ),
        in_specs=[pl.BlockSpec(memory_space=pl.ANY)] * 5,
        out_specs=(pl.BlockSpec(memory_space=vmem),) * 4,
        scratch_shapes=[
            vmem((1, rows), jnp.int32),
            vmem((3, rows), jnp.int32),
            vmem((15, rows), F32),
            vmem((5, 6, cx + 4, yrows, cz), F32),
            vmem((cx, cy, cz), F32),
            vmem((8, 2, cx, 4, cz), F32),
            vmem((8, 2, cx, 4, cz), F32),
            vmem((8, strips, cy, cz), F32),
            vmem((8, 2, strips, cy, cz), F32),
            vmem((2, cx, cy, cz), F32),
            vmem((2, cx, cy, cz), F32),
            vmem((2, 2, 3, cx // 2, 4, cz), F32),
            vmem((wide, cy, cz), F32),
            vmem((2, wide, 2, cz), F32),
            vmem((6, 2, 2, cy, cz), F32),
            vmem((6, 2, cx // 2, 4, cz), F32),
            vmem((6, 2, 2, 4, cz), F32),
            vmem((2, wide, cy, cz), F32),
            vmem((2, 2, cy, cz), F32),
            vmem((2, 2, wide, 2, cz), F32),
            vmem((2, 2, 2, 2, cz), F32),
            vmem((128, rows), F32),
            vmem((2 * cz, cz), BF16),
            vmem((2 * cz, cz), BF16),
            vmem((256, cx * cy + ring + 128 * (wide + 2)), BF16),
            vmem((256, cx * cy + ring + 128), BF16),
            vmem((group, per_owner, 128), F32),
            vmem((group, per_owner, 128), F32),
            vmem((group, 1, 128), F32),
            vmem((slots, 3 * cx * cy), BF16),
            vmem((slots, 3 * outer), BF16),
            vmem((slots, 3 * (cy + 8)), BF16),
            vmem((wide + 2, slots, cz), F32),
            vmem((slots, cz), F32),
            vmem((6, slots, cz), F32),
            vmem((slots, cz), F32),
            pltpu.SemaphoreType.REGULAR((2,)),
            pltpu.SemaphoreType.REGULAR((2,)),
            dma((8,)),
            dma((8, 6)),
            dma((8, 6)),
            dma((2, 26)),
            dma((2, 26)),
            dma((group,)),
            dma((group,)),
            dma((group,)),
            dma((group,)),
        ],
        compiler_params=pltpu.CompilerParams(
            collective_id=0, has_side_effects=True, vmem_limit_bytes=60 * 1024 * 1024
        ),
    )(fields, permittivity, donor_owner.T, donor_base.T, donor_weights.T)
    return pl.pallas_call(
        functools.partial(finish_kernel, cap),
        out_shape=(
            jax.ShapeDtypeStruct(fields.shape, F32),
            jax.ShapeDtypeStruct((6, rows), F32),
        ),
        in_specs=[pl.BlockSpec(memory_space=vmem)] * 4,
        out_specs=(pl.BlockSpec(memory_space=pl.ANY),) * 2,
        scratch_shapes=[vmem((6, rows), F32), dma((2,))],
        compiler_params=pltpu.CompilerParams(vmem_limit_bytes=2 * 1024 * 1024),
    )(new, *answers)


def solution(mesh):
    sizes = (mesh.shape["gx"], mesh.shape["gy"], mesh.shape["gz"])
    placed = (
        P(None, "gx", "gy", "gz"),
        P("gx", "gy", "gz"),
        P(("gx", "gy", "gz"), None),
        P(("gx", "gy", "gz"), None),
        P(("gx", "gy", "gz"), None),
    )
    return jax.shard_map(
        functools.partial(local, sizes),
        mesh=mesh,
        in_specs=placed,
        out_specs=(P(None, "gx", "gy", "gz"), P(None, ("gx", "gy", "gz"))),
        check_vma=False,
    )
```

```python
import functools

import jax
import jax.numpy as jnp
from jax import lax
from jax.experimental import pallas as pl
from jax.experimental.pallas import tpu as pltpu
from jax.sharding import PartitionSpec as P

step_size = 0.25
MESH = pl.DeviceIdType.MESH
F32 = jnp.float32
BF16 = jnp.bfloat16
HI = lax.Precision.HIGHEST
BLOCKS = 4
FEATURES = 32
DIRS = [(a, b, c) for a in (-1, 0, 1) for b in (-1, 0, 1) for c in (-1, 0, 1) if (a, b, c) != (0, 0, 0)]
FACES = [(-1, 0, 0), (1, 0, 0), (0, -1, 0), (0, 1, 0), (0, 0, -1), (0, 0, 1)]


def dot(a, b, dims=((1,), (0,))):
    return lax.dot_general(a, b, (dims, ((), ())), precision=HI, preferred_element_type=F32)


def split(a):
    hi = a.astype(BF16)
    return hi, (a - hi.astype(F32)).astype(BF16)


def dot16(a, b):
    return lax.dot_general(a, b, (((1,), (0,)), ((), ())), preferred_element_type=F32)


def negate(way):
    return tuple(-a for a in way)


def slot_of(a):
    return 0 if a < 0 else 1


def kernel(
    sizes, W_ring, fields, eps, owner_in, bases_in, weights_in, F, ansr, hits_t, slot_t,
    owner, bases, weights, T, inv, ys, yr, zs, zr, DZ, R,
    yfs, zfs, zys, XR, YR, XYR, ZR, ZX, ZY, ZXY,
    data_t, inner, gather, EX, EY, req, reqr, ans, W, V, Wy, wzx, wz_in, part, saved,
    z_sem, y_sem, load_sem, send, recv, fsend, frecv, rsend, rrecv, asend, arecv,
):
    nx, ny, nz, cap = sizes
    group = ny * nz
    per_owner = cap // BLOCKS
    cx, cy, cz = eps.shape
    rows = owner.shape[1]
    slots = group * cap
    x, y, z = lax.axis_index("gx"), lax.axis_index("gy"), lax.axis_index("gz")
    me = y * nz + z
    y0, y1 = 8, 8 + cy

    loads = [
        pltpu.make_async_copy(fields.at[pl.ds(3, 3)], T.at[0, pl.ds(3, 3), pl.ds(2, cx), pl.ds(8, cy), :], load_sem.at[0]),
        pltpu.make_async_copy(owner_in, owner, load_sem.at[1]),
        pltpu.make_async_copy(bases_in, bases, load_sem.at[2]),
        pltpu.make_async_copy(weights_in, weights, load_sem.at[3]),
        pltpu.make_async_copy(eps, inv, load_sem.at[4]),
        pltpu.make_async_copy(fields, F, load_sem.at[5]),
        pltpu.make_async_copy(fields.at[pl.ds(0, 3)], T.at[0, pl.ds(0, 3), pl.ds(2, cx), pl.ds(8, cy), :], load_sem.at[6]),
    ]
    for copy in (loads[0], loads[6], *loads[1:5]):
        copy.start()

    has = {
        (-1, 0, 0): x > 0, (1, 0, 0): x < nx - 1, (0, -1, 0): y > 0,
        (0, 1, 0): y < ny - 1, (0, 0, -1): z > 0, (0, 0, 1): z < nz - 1,
    }
    for way in DIRS:
        found = None
        for axis in range(3):
            if way[axis]:
                face = tuple(way[a] if a == axis else 0 for a in range(3))
                found = has[face] if found is None else found & has[face]
        has[way] = found

    def dev(way):
        return (x + way[0], y + way[1], z + way[2])

    barrier = pltpu.get_barrier_semaphore()
    others = []
    for d in range(1, group):
        t = lax.rem(me + d, group)
        others.append((x, t // nz, lax.rem(t, nz)))
    expected = jnp.int32(0)
    for way in FACES:
        expected = expected + has[way].astype(jnp.int32)

        @pl.when(has[way])
        def _():
            pl.semaphore_signal(barrier, inc=1, device_id=dev(way), device_id_type=MESH)

    def line_stage(k, at, count, sems, up):
        down = negate(up)
        for here, side, way in ((at == k, 0, up), (at == count - 1 - k, 1, down)):
            @pl.when(here)
            def _():
                if k > 0:
                    pl.semaphore_wait(sems.at[side], 1)
                if k < count - 1:
                    pl.semaphore_signal(sems.at[side], inc=1, device_id=dev(way), device_id_type=MESH)

    def z_stage(k):
        line_stage(k, z, nz, z_sem, (0, 0, 1))

    def y_stage(k):
        line_stage(k, y, ny, y_sem, (0, 1, 0))

    lane = lax.broadcasted_iota(jnp.int32, (cy, cz), 1)
    lane1 = lax.broadcasted_iota(jnp.int32, (1, cz), 1)

    def remote(src, dst, s, r, target):
        return pltpu.make_async_remote_copy(
            src_ref=src, dst_ref=dst, send_sem=s, recv_sem=r, device_id=target, device_id_type=MESH)

    def request(d):
        return remote(req.at[(me + d) % group], reqr.at[me], rsend.at[d], rrecv.at[d], others[d - 1])

    def answer(d):
        return remote(ans.at[(me + d) % group], ansr.at[me], asend.at[d], arecv.at[d], others[d - 1])

    def parts(h):
        m = h // 2
        sp = (m + h % 2) % 2
        return m, sp, 3 * (1 - sp), 3 * sp

    def face_copy(h, way):
        m, sp, s, d = parts(h)
        i = FACES.index(way)
        if way[0]:
            lo_src, lo_dst = (2, cx + 2) if way[0] < 0 else (cx, 0)
            src = T.at[m, pl.ds(s + 1, 2), pl.ds(lo_src, 2), pl.ds(8, cy)]
            dst = T.at[m, pl.ds(s + 1, 2), pl.ds(lo_dst, 2), pl.ds(8, cy)]
        elif way[1]:
            k = slot_of(way[1])
            src, dst = ys.at[h, k], yr.at[h, 1 - k]
        else:
            src, dst = zs.at[h], zr.at[h, 1 - slot_of(way[2])]
        return remote(src, dst, send.at[h, i], recv.at[h, i], dev(way))

    def start_face(h, ways, also=None):
        for way in ways:
            @pl.when(has[way] if also is None else has[way] & also)
            def _():
                face_copy(h, way).start()

    def recv_face(h, ways):
        for way in ways:
            @pl.when(has[negate(way)])
            def _():
                face_copy(h, way).wait_recv()

    XW, YW, ZW = FACES[0:2], FACES[2:4], FACES[4:6]
    per = cz // 8

    def pack_y(h):
        m, sp, s, d = parts(h)
        for q, c in enumerate((0, 2)):
            ys[h, 0, :, 2 * q:2 * q + 2, :] = T[m, s + c, 2:2 + cx, y0:y0 + 2, :]
            ys[h, 1, :, 2 * q:2 * q + 2, :] = T[m, s + c, 2:2 + cx, y1 - 2:y1, :]

    def pack_z(h):
        m, sp, s, d = parts(h)
        for g in range(cx // per):
            strip = jnp.zeros((cy, cz), F32)
            for i in range(per):
                for q in range(2):
                    b = i * 8 + q * 4
                    strip = jnp.where(lane // 4 == b // 4,
                                      pltpu.roll(T[m, s + q, 2 + g * per + i, y0:y1, :], (b + 2) % cz, 1), strip)
            zs[h, g] = strip

    loads[0].wait()
    pack_y(0)
    pl.semaphore_wait(barrier, expected)
    for h in range(2):
        if h == 1:
            loads[6].wait()
            loads[5].start()
            pack_y(h)
        start_face(h, XW, y % 2 == 0)
        start_face(h, YW)
        pack_z(h)
        start_face(h, ZW)
        start_face(h, XW, y % 2 == 1)
    z_stage(0)

    def clear(ref):
        ref[...] = jnp.zeros(ref.shape, F32)

    for way in DIRS:
        kx, ky, kz = (slot_of(a) for a in way)
        here = tuple(abs(a) for a in way)

        @pl.when(jnp.logical_not(has[way]))
        def _():
            if here == (1, 0, 0):
                for m in range(4):
                    clear(T.at[m, :, pl.ds(kx * (cx + 2), 2), pl.ds(8, cy)])
                clear(XR.at[:, kx])
            elif here == (0, 1, 0):
                clear(yr.at[:, ky])
                clear(YR.at[:, ky])
            elif here == (0, 0, 1):
                clear(zr.at[:, kz])
                clear(ZR.at[kz])
            elif here == (1, 1, 0):
                clear(XYR.at[:, kx, ky])
            elif here == (1, 0, 1):
                clear(ZX.at[kx, kz])
            elif here == (0, 1, 1):
                clear(ZY.at[ky, kz])
            else:
                clear(ZXY.at[kx, ky, kz])

    zi = lax.broadcasted_iota(jnp.int32, (2 * cz, cz), 0) % cz
    zo = lax.broadcasted_iota(jnp.int32, (2 * cz, cz), 1)
    delta = zi - zo
    inner[...] = (jnp.where(delta == -2, 1.0, 0.0) - jnp.where(delta == 2, 1.0, 0.0)
                  + jnp.where(delta == 1, 8.0, 0.0) - jnp.where(delta == -1, 8.0, 0.0)).astype(BF16)

    for copy in loads[1:4]:
        copy.wait()
    for b in range(BLOCKS):
        at = b * FEATURES
        data_t[at:at + 3] = bases[...].astype(F32)
        data_t[at + 3:at + 18] = weights[...]
        data_t[at + 18:at + FEATURES] = jnp.zeros((FEATURES - 18, rows), F32)
    own = owner[...]
    hits = jnp.where(lax.broadcasted_iota(jnp.int32, (group, rows), 0) == own, 1.0, 0.0)
    hits_t[...] = hits
    earlier = dot16(hits.astype(BF16), (lax.broadcasted_iota(jnp.int32, (rows, rows), 0)
                                        < lax.broadcasted_iota(jnp.int32, (rows, rows), 1)).astype(BF16))
    slot_f = jnp.sum(earlier * hits, axis=0, keepdims=True)
    slot_t[...] = slot_f
    slot = slot_f.astype(jnp.int32)
    block = lax.broadcasted_iota(jnp.int32, (BLOCKS * FEATURES, rows), 0) // FEATURES
    placed = jnp.where(block == slot // per_owner, data_t[...], 0.0)
    flat = own * per_owner + slot % per_owner
    perm = (flat == lax.broadcasted_iota(jnp.int32, (group * per_owner, rows), 0)).astype(F32)
    packed = dot(perm, placed, ((1,), (1,)))
    for o in range(group):
        req[o] = packed[o * per_owner:(o + 1) * per_owner]
    reqr[me] = req[me]
    loads[4].wait()
    inv[...] = 1.0 / (12.0 * inv[...])
    loads[5].wait()
    here_x = lax.broadcasted_iota(jnp.int32, (64, 128), 0)
    inside = cx * cy
    ring_x, ring_y = 4 * cy, 4 * cx

    def one_hot(ref, lo, hot):
        hot = jnp.where(hot, 1.0, 0.0).astype(BF16)
        for k in range(3):
            ref[k * 64:(k + 1) * 64, lo:lo + 128] = hot
        ref[192:256, lo:lo + 128] = jnp.zeros((64, 128), BF16)

    def place(lo, xe, ye):
        one_hot(EX, lo, here_x == xe)
        one_hot(EY, lo, here_x - 32 == ye)

    for lo in range(0, inside, 128):
        li = lo + lane1
        place(lo, li // cy + 2, li % cy + 2)
    for lo in range(0, W_ring, 128):
        li = lo + lane1
        i1 = li % (2 * cy)
        l2 = li - ring_x
        l3 = li - ring_x - ring_y
        xe = jnp.where(
            l2 < 0, i1 // cy + jnp.where(li >= 2 * cy, cx + 2, 0),
            jnp.where(l3 < 0, (l2 % (2 * cx)) // 2 + 2, (l3 % 4) // 2 + jnp.where(l3 >= 8, cx + 2, 0)))
        ye = jnp.where(
            l2 < 0, i1 % cy + 2,
            jnp.where(l3 < 0, l2 % 2 + jnp.where(l2 >= 2 * cx, cy + 2, 0),
                      l3 % 2 + jnp.where(l3 % 8 >= 4, cy + 2, 0)))
        place(inside + lo, jnp.where(l3 < 16, xe, -100), jnp.where(l3 < 16, ye, -100))
    ye = jnp.where(lane1 < cy, lane1 + 2, jnp.where(lane1 < cy + 2, lane1 - cy, lane1))
    one_hot(EY, inside + W_ring, here_x - 32 == jnp.where(lane1 < cy + 4, ye, -100))
    wide = cz // 32
    for g in range(wzx.shape[0]):
        xe = lane1 // 32 + 2 + wide * (g - 1)
        one_hot(EX, inside + W_ring + 128 * g, here_x == jnp.where(xe < 32, xe, -100))
    comp_row = lax.broadcasted_iota(jnp.int32, (2 * cz, cz), 0) % 32 // 4
    comp_col = lax.broadcasted_iota(jnp.int32, (2 * cz, cz), 1) // cap
    gather[...] = jnp.where((comp_row == comp_col) & (comp_row < 6), 1.0, 0.0).astype(BF16)
    for k in range(1, min(2, nz)):
        z_stage(k)

    edge = (lane < 2) | (lane >= cz - 2)
    tail = lane % 4

    def final_copy(j, way):
        i = DIRS.index(way)
        d = 3 * (1 - j)
        here = tuple(abs(a) for a in way)
        kx, ky, kz = (slot_of(a) for a in way)
        nx_, ny_, nz_ = 1 - kx, 1 - ky, 1 - kz
        strip = kx * (zfs.shape[0] - 1)
        if here == (1, 0, 0):
            src, dst = F.at[pl.ds(d, 3), pl.ds(kx * (cx - 2), 2)], XR.at[pl.ds(d, 3), nx_]
        elif here == (0, 1, 0):
            src, dst = yfs.at[j, ky], YR.at[pl.ds(d, 3), ny_]
        elif here == (0, 0, 1):
            src, dst = zfs, ZR.at[nz_]
        elif here == (1, 1, 0):
            src = yfs.at[j, ky, :, kx * (cx // 2 - 1)]
            dst = XYR.at[pl.ds(d, 3), nx_, ny_]
        elif here == (1, 0, 1):
            src, dst = zfs.at[strip], ZX.at[nx_, nz_]
        elif here == (0, 1, 1):
            src, dst = zys.at[ky], ZY.at[ny_, nz_]
        else:
            src, dst = zys.at[ky, strip], ZXY.at[nx_, ny_, nz_]
        return remote(src, dst, fsend.at[j, i], frecv.at[j, i], dev(way))

    def start_final(j, ways, also=None):
        for way in ways:
            @pl.when(has[way] if also is None else has[way] & also)
            def _():
                final_copy(j, way).start()

    served_rows = group * per_owner

    def served_table():
        if per_owner % 8 == 0:
            table = reqr[...].reshape(served_rows, 128)
        else:
            table = jnp.concatenate([reqr[o] for o in range(group)], axis=0)
        turned = [table] + [pltpu.roll(table, 128 - b * FEATURES, 1) for b in range(1, BLOCKS)]
        return jnp.concatenate(turned, axis=0)

    def build():
        for d in range(1, group):
            request(d).wait_recv()
        served = served_table()

        def column(k):
            return jnp.broadcast_to(served[:, k:k + 1], (slots, 128))

        li = lax.broadcasted_iota(jnp.int32, (slots, 128), 1)
        flat_lane = li.astype(F32)
        bx, by, bz = column(0), column(1), column(2)
        in_x, in_xy = li < 32, li < 64
        off = jnp.where(in_x, flat_lane - bx, flat_lane - 32.0 - by)
        t = li % 4
        off_z = flat_lane + 2.0 - bz
        off_t = jnp.where(t < 2, t, cz + t).astype(F32) - bz
        both = jnp.zeros((slots, 128), F32)
        z_in = jnp.zeros((slots, 128), F32)
        tails = jnp.zeros((slots, 128), F32)
        for k in range(5):
            wz = column(13 + k)
            both = jnp.where(off == k, jnp.where(in_x, column(3 + k), column(8 + k)), both)
            z_in = jnp.where(off_z == k, wz, z_in)
            tails = jnp.where(off_t == k, wz, tails)
        wz_in[...] = z_in
        both = jnp.where(in_xy, both, 0.0)
        hi = both.astype(BF16).astype(F32)
        mid = (both - hi).astype(BF16).astype(F32)
        table = jnp.concatenate([(hi + pltpu.roll(mid, 64, 1)).astype(BF16), (both - hi - mid).astype(BF16)], axis=1)

        def weights_at(lo, n):
            return dot16(table, EX[:, lo:lo + n]) * dot16(table, EY[:, lo:lo + n])

        hi, lo = split(weights_at(0, inside))
        for k, piece in enumerate((hi, hi, lo)):
            W[:, k * inside:(k + 1) * inside] = piece
        n = V.shape[1] // 3
        hi, lo = split(weights_at(inside, W_ring))
        for k, piece in enumerate((hi, hi, lo)):
            V[:, k * n:(k + 1) * n] = piece[:, 0:n]
        k = cy + 8
        hi, lo = split(dot16(table, EY[:, inside + W_ring:inside + W_ring + 128]))
        Wy[:, 0:k] = hi[:, 0:k]
        Wy[:, k:2 * k] = hi[:, 0:k]
        Wy[:, 2 * k:3 * k] = lo[:, 0:k]
        at_x = dot16(table, EX[:, inside + W_ring:])
        for g in range(wzx.shape[0]):
            wzx[g] = tails * at_x[:, g * 128:(g + 1) * 128]

    z_ways = sorted((way for way in DIRS if way[2]), key=lambda way: -sum(map(abs, way)))
    flat_ways = [way for way in DIRS if way[0] and way[1] and not way[2]] + YW

    def half(h, last):
        m, sp, s, d = parts(h)
        hi, lo = split(T[m, pl.ds(s, 2), 2:2 + cx, y0:y1, :].reshape(2 * cx * cy, cz))
        DZ[...] = dot16(jnp.concatenate([hi, lo], axis=1), inner[...]).reshape(2, cx, cy, cz)
        if not last:
            @pl.when(h == 1)
            def _():
                for k in range(2, min(3, nz)):
                    z_stage(k)

            @pl.when(h == 2)
            def _():
                for k in range(3, nz):
                    z_stage(k)
                y_stage(0)

            @pl.when(h == 3)
            def _():
                for k in range(1, min(2, ny)):
                    y_stage(k)

            @pl.when(h == 4)
            def _():
                for k in range(2, ny):
                    y_stage(k)
                for d in range(1, group):
                    request(d).start()

        recv_face(h, YW)
        for q, c in enumerate((0, 2)):
            T[m, s + c, 2:2 + cx, y0 - 2:y0, :] = yr[h, 0, :, 2 * q:2 * q + 2, :]
            T[m, s + c, 2:2 + cx, y1:y1 + 2, :] = yr[h, 1, :, 2 * q:2 * q + 2, :]
        scale = step_size / jnp.asarray(m + 1, F32)
        plain = -scale / 12.0
        strips = [zfs[g] if h == 7 else jnp.zeros((cy, cz), F32) for g in range(cx // wide)] if last else []

        def by_of(px):
            return jnp.where(sp == 0, inv[px] * scale, plain)

        def rates_of(px):
            def d_x(c):
                at = lambda o: T[m, s + c, 2 + px + o, y0:y1, :]
                return (at(-2) - at(2)) + 8.0 * (at(1) - at(-1))

            def d_y(c):
                at = lambda o: T[m, s + c, 2 + px, y0 + o:y1 + o, :]
                return (at(-2) - at(2)) + 8.0 * (at(1) - at(-1))

            return [d_y(2) - DZ[1, px], DZ[0, px] - d_x(2), d_x(1) - d_y(0)]

        def finish_plane(px, rates, by, comps=range(3)):
            for c in comps:
                rate = rates[c] * by
                total = F[d + c, px] + rate
                F[d + c, px] = total
                if last:
                    g, i = px // wide, px % wide
                    b = i * 32 + (d + c) * 4
                    strips[g] = jnp.where(lane // 4 == b // 4, pltpu.roll(total, (b + 2) % cz, 1), strips[g])
                else:
                    T[m + 1, d + c, 2 + px, y0:y1, :] = rate

        for px in range(2, cx - 2):
            rates = rates_of(px)
            for c in range(2):
                R[c, px] = rates[c]
            finish_plane(px, rates, by_of(px), (2,))
        recv_face(h, ZW)
        for g in range(cx // per):
            merged = jnp.where(tail < 2, zr[h, 0, g], zr[h, 1, g])
            l2, r2 = pltpu.roll(merged, cz - 2, 1), pltpu.roll(merged, 2, 1)
            l1, r1 = pltpu.roll(merged, cz - 1, 1), pltpu.roll(merged, 1, 1)
            fix = (jnp.where(tail < 2, -l2, r2)
                   + 8.0 * (jnp.where(tail == 1, l1, 0.0) - jnp.where(tail == 2, r1, 0.0)))

            def at_edge(px, q):
                b = px % per * 8 + q * 4
                return jnp.where(edge, pltpu.roll(fix, (2 * cz - b - 2) % cz, 1), 0.0)

            for px in range(g * per, (g + 1) * per):
                if px in (0, 1, cx - 2, cx - 1):
                    for q in range(2):
                        DZ[q, px] = DZ[q, px] + at_edge(px, q)
                else:
                    finish_plane(px, [R[0, px] - at_edge(px, 1), R[1, px] + at_edge(px, 0)], by_of(px), (0, 1))
        recv_face(h, XW)
        for px in (0, 1, cx - 2, cx - 1):
            finish_plane(px, rates_of(px), by_of(px))
        if last:
            j = h - 6
            for g, strip in enumerate(strips):
                zfs[g] = strip
                if j == 1:
                    zys[0, g] = strip[0:2]
                    zys[1, g] = strip[cy - 2:cy]
            if j == 1:
                start_final(j, z_ways)
            start_final(j, XW, y % 2 == 0)
            for k, lo in ((0, 0), (1, cy - 2)):
                for c in range(3):
                    for px in range(cx):
                        yfs[j, k, c, px // 2, px % 2 * 2:px % 2 * 2 + 2, :] = F[d + c, px, lo:lo + 2, :]
            start_final(j, flat_ways)
            start_final(j, XW, y % 2 == 1)
        else:
            start_face(h + 2, XW, y % 2 == 0)
            pack_y(h + 2)
            start_face(h + 2, YW)
            pack_z(h + 2)
            start_face(h + 2, ZW)
            start_face(h + 2, XW, y % 2 == 1)

    def body(h, carry):
        half(h, False)
        return carry

    lax.fori_loop(0, 6, body, 0)
    half(6, True)
    half(7, True)

    build()
    depth = cx * cy

    def apply(w, block):
        hi, lo = split(block)
        return dot16(w[...], jnp.concatenate([hi, lo, hi], axis=0))

    for d in (3, 0):
        both = apply(W, jnp.concatenate([F[d + c].reshape(depth, cz) for c in range(3)], axis=1))
        for c in range(3):
            part[d + c] = both[:, c * cz:(c + 1) * cz]

    slot_row = lax.broadcasted_iota(jnp.int32, (slots, cz), 0)
    slot_lane = lax.broadcasted_iota(jnp.int32, (slots, cz), 1)
    target = slot_row // served_rows * per_owner + slot_row % per_owner - slot_lane
    result = jnp.zeros((slots, cz), F32)
    ktail = lax.broadcasted_iota(jnp.int32, (1, cz), 1) % 4 < 2
    def faces(j, result):
        d = 3 * (1 - j)
        blocks = []
        for c in range(3):
            pieces = ([XR[d + c].reshape(4 * cy, cz)]
                      + [YR[d + c, k, i] for k in range(2) for i in range(cx // 2)]
                      + [XYR[d + c, kx, ky] for kx in range(2) for ky in range(2)])
            blocks.append(jnp.concatenate(pieces, axis=0))
        added = apply(V, jnp.concatenate(blocks, axis=1))
        for c in range(3):
            both = (part[d + c] + added[:, c * cz:(c + 1) * cz]) * wz_in[...]
            result = jnp.where(target == -(d + c) * cap, jnp.sum(both, axis=1, keepdims=True), result)
        return result

    def recv_final(j, ways):
        for way in ways:
            @pl.when(has[negate(way)])
            def _():
                final_copy(j, way).wait_recv()

    def ring(centre, low, high):
        return jnp.concatenate(
            [jnp.where(ktail, a[0], a[1]) for a in (centre, low, high)] + [jnp.zeros((4, cz), F32)], axis=0)

    recv_final(0, flat_ways + XW)
    saved[...] = faces(0, result)
    recv_final(1, z_ways)
    strips = [ring([ZX[0, k] for k in range(2)], [ZXY[0, 0, k] for k in range(2)],
                   [ZXY[0, 1, k] for k in range(2)])]
    for g in range(cx // wide):
        strips.append(ring([ZR[k, g] for k in range(2)], [ZY[0, k, g] for k in range(2)],
                           [ZY[1, k, g] for k in range(2)]))
    strips.append(ring([ZX[1, k] for k in range(2)], [ZXY[1, 0, k] for k in range(2)],
                       [ZXY[1, 1, k] for k in range(2)]))
    hi, lo = split(jnp.concatenate(strips, axis=1))
    zsum = dot16(Wy[...], jnp.concatenate([hi, lo, hi], axis=0))
    zpart = jnp.zeros((slots, cz), F32)
    for g in range(len(strips)):
        zpart = zpart + zsum[:, g * cz:(g + 1) * cz] * wzx[g]
    zsum = dot16(jnp.concatenate(split(zpart), axis=1), gather[...])
    saved[...] = saved[...] + jnp.where((target + slot_lane) == slot_lane % cap, zsum, 0.0)
    recv_final(1, flat_ways + XW)
    result = saved[...] + faces(1, result)

    folded = result[0:served_rows]
    for b in range(1, BLOCKS):
        folded = folded + result[b * served_rows:(b + 1) * served_rows]
    for o in range(group):
        ans[o] = jnp.sum(folded[o * per_owner:(o + 1) * per_owner], axis=0, keepdims=True)
    for d in range(1, group):
        answer(d).start()
    ansr[me] = ans[me]

    def drain(h, carry):
        for way in FACES:
            @pl.when(has[way])
            def _():
                face_copy(h, way).wait_send()
        return carry

    lax.fori_loop(0, 8, drain, 0)
    for j in range(2):
        for way in DIRS:
            if j == 1 or not way[2]:
                @pl.when(has[way])
                def _():
                    final_copy(j, way).wait_send()
    for d in range(1, group):
        request(d).wait_send()
    for d in range(1, group):
        answer(d).wait_recv()
    for d in range(1, group):
        answer(d).wait_send()


def finish_kernel(cap, F, ansr, hits_t, slot_t, out, recept, values, sem):
    store = pltpu.make_async_copy(F, out, sem.at[0])
    store.start()
    group = ansr.shape[0]
    got = jnp.concatenate([ansr[o] for o in range(group)], axis=0)
    hi, low = split(got)
    mid, lo = split(got - hi.astype(F32))
    hits = hits_t[...].astype(BF16)
    picked = lax.dot_general(jnp.concatenate([hi, mid, lo], axis=0), jnp.concatenate([hits] * 3, axis=0),
                             (((0,), (0,)), ((), ())), preferred_element_type=F32)
    at = lax.broadcasted_iota(jnp.int32, picked.shape, 0) % cap
    picked = jnp.where(at == slot_t[...].astype(jnp.int32), picked, 0.0)
    for c in range(6):
        values[c:c + 1] = jnp.sum(picked[c * cap:(c + 1) * cap], axis=0, keepdims=True)
    small = pltpu.make_async_copy(values, recept, sem.at[1])
    small.start()
    store.wait()
    small.wait()


def local(sizes, fields, permittivity, donor_owner, donor_base, donor_weights):
    nx, ny, nz = sizes
    cx, cy, cz = permittivity.shape
    rows = donor_owner.shape[0]
    group = ny * nz
    cap = 2 * rows // group
    slots = group * cap
    per_owner = cap // BLOCKS
    vmem = pltpu.VMEM
    dma = pltpu.SemaphoreType.DMA
    yrows = cy + 16
    strips = cx * 8 // cz
    wide = cx * 32 // cz
    outer = 4 * cy + 4 * cx + 16
    ring = -(-outer // 128) * 128
    new, *answers = pl.pallas_call(
        functools.partial(kernel, (nx, ny, nz, cap), ring),
        out_shape=(
            vmem(fields.shape, F32),
            vmem((group, 1, 128), F32),
            vmem((group, rows), F32),
            vmem((1, rows), F32),
        ),
        in_specs=[pl.BlockSpec(memory_space=pl.ANY)] * 5,
        out_specs=(pl.BlockSpec(memory_space=vmem),) * 4,
        scratch_shapes=[
            vmem((1, rows), jnp.int32),
            vmem((3, rows), jnp.int32),
            vmem((15, rows), F32),
            vmem((5, 6, cx + 4, yrows, cz), F32),
            vmem((cx, cy, cz), F32),
            vmem((8, 2, cx, 4, cz), F32),
            vmem((8, 2, cx, 4, cz), F32),
            vmem((8, strips, cy, cz), F32),
            vmem((8, 2, strips, cy, cz), F32),
            vmem((2, cx, cy, cz), F32),
            vmem((2, cx, cy, cz), F32),
            vmem((2, 2, 3, cx // 2, 4, cz), F32),
            vmem((wide, cy, cz), F32),
            vmem((2, wide, 2, cz), F32),
            vmem((6, 2, 2, cy, cz), F32),
            vmem((6, 2, cx // 2, 4, cz), F32),
            vmem((6, 2, 2, 4, cz), F32),
            vmem((2, wide, cy, cz), F32),
            vmem((2, 2, cy, cz), F32),
            vmem((2, 2, wide, 2, cz), F32),
            vmem((2, 2, 2, 2, cz), F32),
            vmem((128, rows), F32),
            vmem((2 * cz, cz), BF16),
            vmem((2 * cz, cz), BF16),
            vmem((256, cx * cy + ring + 128 * (wide + 2)), BF16),
            vmem((256, cx * cy + ring + 128), BF16),
            vmem((group, per_owner, 128), F32),
            vmem((group, per_owner, 128), F32),
            vmem((group, 1, 128), F32),
            vmem((slots, 3 * cx * cy), BF16),
            vmem((slots, 3 * outer), BF16),
            vmem((slots, 3 * (cy + 8)), BF16),
            vmem((wide + 2, slots, cz), F32),
            vmem((slots, cz), F32),
            vmem((6, slots, cz), F32),
            vmem((slots, cz), F32),
            pltpu.SemaphoreType.REGULAR((2,)),
            pltpu.SemaphoreType.REGULAR((2,)),
            dma((8,)),
            dma((8, 6)),
            dma((8, 6)),
            dma((2, 26)),
            dma((2, 26)),
            dma((group,)),
            dma((group,)),
            dma((group,)),
            dma((group,)),
        ],
        compiler_params=pltpu.CompilerParams(
            collective_id=0, has_side_effects=True, vmem_limit_bytes=60 * 1024 * 1024
        ),
    )(fields, permittivity, donor_owner.T, donor_base.T, donor_weights.T)
    return pl.pallas_call(
        functools.partial(finish_kernel, cap),
        out_shape=(
            jax.ShapeDtypeStruct(fields.shape, F32),
            jax.ShapeDtypeStruct((6, rows), F32),
        ),
        in_specs=[pl.BlockSpec(memory_space=vmem)] * 4,
        out_specs=(pl.BlockSpec(memory_space=pl.ANY),) * 2,
        scratch_shapes=[vmem((6, rows), F32), dma((2,))],
        compiler_params=pltpu.CompilerParams(vmem_limit_bytes=2 * 1024 * 1024),
    )(new, *answers)


def solution(mesh):
    sizes = (mesh.shape["gx"], mesh.shape["gy"], mesh.shape["gz"])
    placed = (
        P(None, "gx", "gy", "gz"),
        P("gx", "gy", "gz"),
        P(("gx", "gy", "gz"), None),
        P(("gx", "gy", "gz"), None),
        P(("gx", "gy", "gz"), None),
    )
    return jax.shard_map(
        functools.partial(local, sizes),
        mesh=mesh,
        in_specs=placed,
        out_specs=(P(None, "gx", "gy", "gz"), P(None, ("gx", "gy", "gz"))),
        check_vma=False,
    )
```
